256 devices in a mesh: scan: 128 (over y_hi, x, z, core), tile: 2 (over y_lo).
Axes of the slice: x: 4, y: 4 (y_hi: 2, y_lo: 2; y = y_hi * 2 + y_lo), z: 8, core: 2. Of those that a mesh axis runs over, the one named last changes fastest.
Arguments:
- probe_modes: float32 [12, 2, 128, 128], replicated, may hold values from -5 to 5
- patterns: float32 [1024, 128, 128], P(('scan', 'tile')), may hold values from 0.005 to 300
- specimen: float32 [2, 16384, 512], P(None, 'scan', 'tile'), may hold values from -17.5 to 17.5
- offsets: int32 [1024, 2], P(('scan', 'tile')), may hold values from -128 to 16384, as said below
Outputs:
- new_probe: float32 [12, 2, 128, 128], replicated
- new_specimen: float32 [2, 16384, 512], P(None, 'scan', 'tile')
The draws below stay inside these ranges and needn't reach their ends.
Inputs may be any that keep to these rules, and one draw needn't show every extreme that they name: `offsets`: position p lies in aligned block b = p // 4, held by the device of scan index s = b // (the number of tile devices) and tile index t = b % (the number of tile devices); its row offset lies in s * 128 - 128 to s * 128 + 128, its column offset in t * 256 - 128 to t * 256 + 256, both ends included; in every block one position has its row offset at the lower end and its column offset at the upper end, and one has its row offset at the upper end.
All inputs are finite; a program needn't handle non-finite values.
Results may differ from the reference program's by a relative error of at most 0.0001.
Values sent between devices are 32-bit elements; how exact they have to be, the bound alone decides.
A program may use at most 64 MiB of HBM per device.

```python
import math
import jax
import jax.numpy as jnp
from jax import lax

DET = 128
MODES = 12
P_DEV = 4
ROWS_DEV = 128
COLS_DEV = 256
NS_STEPS = 8
POSITIONS = 1024
OBJ_ROWS = 16384
OBJ_COLS = 512


def draw_probe_modes(key, part):
    key_base, key_weight = jax.random.split(key, 2)
    shape_all = (MODES, 2, DET, DET)
    base_field = jnp.clip(jax.random.normal(key_base, shape_all, jnp.float32), -5.0, 5.0)
    weights = jnp.exp(jax.random.uniform(key_weight, (MODES,), jnp.float32, math.log(0.1), math.log(0.4)))
    mixing = 0.6
    weights = weights.at[0].set(1.0)
    mixed = base_field + mixing * base_field[0:1]
    mixed = mixed.at[0].set(base_field[0])
    return (mixed * weights[:, None, None, None]).astype(jnp.float32)


def draw_patterns(key, part):
    key_flux, key_pixel, key_speckle = jax.random.split(key, 3)
    block_count = POSITIONS // P_DEV
    along = (jnp.arange(POSITIONS, dtype=jnp.int32) // P_DEV).astype(jnp.float32) / max(block_count - 1, 1)
    flux_low, flux_high, growth, speck_low, speck_high = (1.0, 6.0, 3.0, 0.2, 1.8)
    flux = jnp.exp(jax.random.uniform(key_flux, (POSITIONS,), jnp.float32, math.log(flux_low), math.log(flux_high))) * growth ** along
    pixel_gain = jnp.exp(jax.random.uniform(key_pixel, (DET, DET), jnp.float32, math.log(0.3), math.log(3.0)))
    speckle = jax.random.uniform(key_speckle, (POSITIONS, DET, DET), jnp.float32, speck_low, speck_high)
    return (flux[:, None, None] * pixel_gain[None] * speckle).astype(jnp.float32)


def draw_specimen(key, part):
    key_values, key_rows, key_cols = jax.random.split(key, 3)
    values = 0.4 * jnp.clip(jax.random.normal(key_values, (2, OBJ_ROWS, OBJ_COLS), jnp.float32), -4.0, 4.0)
    mean_part = 1.0
    row_scale = jnp.exp(jax.random.uniform(key_rows, (OBJ_ROWS,), jnp.float32, math.log(0.5), math.log(2.0)))
    col_scale = jnp.exp(jax.random.uniform(key_cols, (OBJ_COLS,), jnp.float32, math.log(0.5), math.log(2.0)))
    rough = values * row_scale[None, :, None] * col_scale[None, None, :]
    shift = jnp.array([mean_part, 0.0], jnp.float32)[:, None, None]
    return (rough + shift).astype(jnp.float32)


def draw_offsets(key, part):
    key_rows, key_cols = jax.random.split(key, 2)
    tile_count = OBJ_COLS // COLS_DEV
    position = jnp.arange(POSITIONS, dtype=jnp.int32)
    group_index = position // P_DEV
    within = position % P_DEV
    scan_index = group_index // tile_count
    tile_index = group_index % tile_count
    local_row = jax.random.randint(key_rows, (POSITIONS,), 0, ROWS_DEV + DET + 1, dtype=jnp.int32)
    local_col = jax.random.randint(key_cols, (POSITIONS,), 0, COLS_DEV + DET + 1, dtype=jnp.int32)
    local_row = jnp.where(within == 0, 0, jnp.where(within == 1, ROWS_DEV + DET, local_row))
    local_col = jnp.where(within == 0, COLS_DEV + DET, local_col)
    row_offsets = scan_index * ROWS_DEV - DET + local_row
    col_offsets = tile_index * COLS_DEV - DET + local_col
    return jnp.stack([row_offsets, col_offsets], axis=1).astype(jnp.int32)


def setup_inputs(seed: int = 0) -> dict:
    splits = jax.random.split(jax.random.key(seed), 5)
    return {
        "probe_modes": draw_probe_modes(jax.random.fold_in(splits[4], 71), 0),
        "patterns": draw_patterns(jax.random.fold_in(splits[4], 71), 0),
        "specimen": draw_specimen(jax.random.fold_in(splits[4], 71), 0),
        "offsets": draw_offsets(jax.random.fold_in(splits[4], 71), 0),
    }


highest = lax.Precision.HIGHEST
light_floor = 0.05
object_reg = 0.5
probe_reg = 1.0
total_eps = 1e-06

def newton_steps(gram_re, gram_im):
    mode_count = gram_re.shape[0]
    upper = jnp.concatenate([gram_re, -gram_im], axis=1)
    lower = jnp.concatenate([gram_im, gram_re], axis=1)
    embedded = jnp.concatenate([upper, lower], axis=0)
    frobenius = jnp.sqrt(jnp.sum(embedded * embedded))
    identity = jnp.eye(2 * mode_count, dtype=jnp.float32)
    current = embedded / frobenius
    inverse = identity
    for repeat in range(NS_STEPS):
        factor = 1.5 * identity - 0.5 * jnp.dot(inverse, current, precision=highest, preferred_element_type=jnp.float32)
        current = jnp.dot(current, factor, precision=highest, preferred_element_type=jnp.float32)
        inverse = jnp.dot(factor, inverse, precision=highest, preferred_element_type=jnp.float32)
    inverse = inverse / jnp.sqrt(frobenius)
    return (inverse[:mode_count, :mode_count], inverse[mode_count:, :mode_count])

def gram_parts(mode_rows):
    real_rows = mode_rows[0::2]
    imag_rows = mode_rows[1::2]
    gram_re = jnp.dot(real_rows, real_rows.T, precision=highest, preferred_element_type=jnp.float32) + jnp.dot(imag_rows, imag_rows.T, precision=highest, preferred_element_type=jnp.float32)
    gram_im = jnp.dot(real_rows, imag_rows.T, precision=highest, preferred_element_type=jnp.float32) - jnp.dot(imag_rows, real_rows.T, precision=highest, preferred_element_type=jnp.float32)
    return (gram_re, gram_im)

def orthonormal_rows(mode_rows, gram_re, gram_im, power_ratio):
    real_rows = mode_rows[0::2]
    imag_rows = mode_rows[1::2]
    mix_re, mix_im = newton_steps(gram_re, gram_im)
    ortho_re = jnp.dot(mix_re.T, real_rows, precision=highest, preferred_element_type=jnp.float32) - jnp.dot(mix_im.T, imag_rows, precision=highest, preferred_element_type=jnp.float32)
    ortho_im = jnp.dot(mix_im.T, real_rows, precision=highest, preferred_element_type=jnp.float32) + jnp.dot(mix_re.T, imag_rows, precision=highest, preferred_element_type=jnp.float32)
    weight = jnp.sqrt(power_ratio * jnp.diagonal(gram_re))
    joined = jnp.stack([ortho_re, ortho_im], axis=1) * weight[:, None, None]
    return joined.reshape(mode_rows.shape)

def reference(probe_modes, patterns, specimen, offsets):
    detector = probe_modes.shape[-1]
    mode_count = probe_modes.shape[0]
    probe_field = lax.complex(probe_modes[:, 0], probe_modes[:, 1])
    probe_power = lax.optimization_barrier(jnp.sum(probe_modes[:, 0] ** 2 + probe_modes[:, 1] ** 2, axis=0))
    padded = jnp.pad(lax.complex(specimen[0], specimen[1]), ((detector, detector), (detector, detector)))
    frame_zeros = jnp.zeros(padded.shape, jnp.float32)
    mode_zeros = jnp.zeros((mode_count, detector, detector), jnp.float32)

    def one_position(position, running):
        grad_sum, light_sum, frame_num, frame_light, model_sum = running
        row_at = (offsets[position, 0] + detector).astype(jnp.int32)
        col_at = (offsets[position, 1] + detector).astype(jnp.int32)
        patch_now = lax.dynamic_slice(padded, (row_at, col_at), (detector, detector))
        exit_wave = probe_field * patch_now[None]
        model_sum = model_sum + jnp.sum(jnp.real(exit_wave) ** 2 + jnp.imag(exit_wave) ** 2)
        far_field = jnp.fft.fft2(exit_wave, norm='ortho')
        model_light = lax.optimization_barrier(jnp.sum(jnp.real(far_field) ** 2 + jnp.imag(far_field) ** 2, axis=0))
        factor = jnp.sqrt(patterns[position]) / jnp.sqrt(jnp.maximum(model_light, light_floor)) - 1.0
        change = jnp.fft.ifft2(far_field * factor[None], norm='ortho')
        grad_sum = grad_sum + jnp.conj(patch_now)[None] * change
        light_sum = light_sum + jnp.real(patch_now) ** 2 + jnp.imag(patch_now) ** 2
        contribution = lax.optimization_barrier(jnp.sum(jnp.conj(probe_field) * change, axis=0))
        old_num = lax.dynamic_slice(frame_num, (row_at, col_at), (detector, detector))
        frame_num = lax.dynamic_update_slice(frame_num, old_num + contribution, (row_at, col_at))
        old_light = lax.dynamic_slice(frame_light, (row_at, col_at), (detector, detector))
        frame_light = lax.dynamic_update_slice(frame_light, old_light + probe_power, (row_at, col_at))
        return (grad_sum, light_sum, frame_num, frame_light, model_sum)
    initial = (lax.complex(mode_zeros, mode_zeros), jnp.zeros((detector, detector), jnp.float32), lax.complex(frame_zeros, frame_zeros), frame_zeros, jnp.zeros((), jnp.float32))
    grad_sum, light_sum, frame_num, frame_light, model_sum = lax.fori_loop(0, POSITIONS, one_position, initial)
    interior_num = frame_num[detector:-detector, detector:-detector]
    interior_light = frame_light[detector:-detector, detector:-detector]
    new_field = padded[detector:-detector, detector:-detector] + interior_num / (interior_light + object_reg)
    new_specimen = jnp.stack([jnp.real(new_field), jnp.imag(new_field)])
    updated = probe_field + grad_sum / (light_sum + probe_reg)[None]
    updated_rows = jnp.stack([jnp.real(updated), jnp.imag(updated)], axis=1).reshape(2 * mode_count, -1)
    power_ratio = jnp.sum(patterns) / (model_sum + total_eps)
    gram_re, gram_im = gram_parts(updated_rows)
    new_rows = orthonormal_rows(updated_rows, gram_re, gram_im, power_ratio)
    return (new_rows.reshape(probe_modes.shape), new_specimen)
```

```python
import math

import jax
import jax.numpy as jnp
import ml_dtypes
import numpy as np
from jax import lax
from jax.experimental import pallas as pl
from jax.experimental.pallas import tpu as pltpu
from jax.sharding import PartitionSpec as P

NS_STEPS = 8
DET = 128
TALL = 136
LIGHT_FLOOR = 0.05
OBJECT_REG = 0.5
PROBE_REG = 1.0
TOTAL_EPS = 1e-06
VMEM = pl.BlockSpec(memory_space=pltpu.VMEM)
SMEM = pl.BlockSpec(memory_space=pltpu.SMEM)
highest = lax.Precision.HIGHEST


def split_tables():
    index = np.arange(DET)
    angles = -2.0 * math.pi / DET * (index[:, None] * index[None, :] % DET)
    cos, sin = np.cos(angles) / math.sqrt(DET), np.sin(angles) / math.sqrt(DET)
    right = np.block([[cos, sin], [-sin, cos]])
    tables = []
    for matrix in (right, right.T):
        high = matrix.astype(ml_dtypes.bfloat16)
        low = (matrix - high.astype(np.float64)).astype(ml_dtypes.bfloat16)
        tables += [high, low]
    return [jnp.asarray(table) for table in tables]


def split(value):
    high = value.astype(jnp.bfloat16)
    return high, (value - high.astype(jnp.float32)).astype(jnp.bfloat16)


def mm(a, b):
    return jnp.dot(a, b, preferred_element_type=jnp.float32)


def window_of(local_ref, position):
    row = local_ref[position, 0]
    col = local_ref[position, 1]
    tile = jnp.minimum(col // DET, 2)
    slab = jnp.minimum(row // 8, 31)
    return pl.multiple_of(slab * 8, 8), row - slab * 8, pl.multiple_of(tile * DET, DET), col - tile * DET


def positions_kernel(
    local_ref,
    probe_ref,
    patterns_ref,
    ext_ref,
    rh_ref,
    rl_ref,
    lh_ref,
    ll_ref,
    sums_ref,
    frame_ref,
    patch_ref,
    far_ref,
    num_ref,
):
    modes = probe_ref.shape[0]
    pairs = modes // 2
    power = jnp.zeros((DET, DET), jnp.float32)
    for k in range(modes):
        power = power + probe_ref[k, 0] * probe_ref[k, 0] + probe_ref[k, 1] * probe_ref[k, 1]
    sums_ref[...] = jnp.zeros_like(sums_ref)
    frame_ref[...] = jnp.zeros_like(frame_ref)

    def one_position(position, _):
        slab, drop, tile, shift = window_of(local_ref, position)
        for c in range(2):
            window = ext_ref[c, pl.ds(slab, TALL), pl.ds(tile, 2 * DET)]
            window = pltpu.roll(window, lax.rem(2 * DET - shift, 2 * DET), 1)[:, :DET]
            patch_ref[c] = pltpu.roll(window, lax.rem(TALL - drop, TALL), 0)[:DET]
        model = jnp.zeros((DET, DET), jnp.float32)
        for j in range(pairs):
            lefts = []
            for k in (2 * j, 2 * j + 1):
                pr, pi = probe_ref[k, 0], probe_ref[k, 1]
                ar, ai = patch_ref[0], patch_ref[1]
                lefts.append(jnp.concatenate([pr * ar - pi * ai, pr * ai + pi * ar], axis=1))
            xh, xl = split(jnp.concatenate(lefts, axis=0))
            half = mm(xh, rh_ref[...]) + mm(xl, rh_ref[...]) + mm(xh, rl_ref[...])
            half = jnp.concatenate(
                [
                    jnp.concatenate([half[:DET, :DET], half[DET:, :DET]], axis=1),
                    jnp.concatenate([half[:DET, DET:], half[DET:, DET:]], axis=1),
                ],
                axis=0,
            )
            yh, yl = split(half)
            far = mm(lh_ref[...], yh) + mm(lh_ref[...], yl) + mm(ll_ref[...], yh)
            far_ref[j] = far
            squares = far * far
            squares = squares[:DET] + squares[DET:]
            model = model + squares[:, :DET] + squares[:, DET:]
        factor = jnp.sqrt(patterns_ref[position]) / jnp.sqrt(jnp.maximum(model, LIGHT_FLOOR)) - 1.0
        wide = jnp.concatenate([factor, factor], axis=1)
        wide = jnp.concatenate([wide, wide], axis=0)
        num_ref[...] = jnp.zeros_like(num_ref)
        for j in range(pairs):
            bh, bl = split(far_ref[j] * wide)
            back = mm(rh_ref[...], bh) + mm(rh_ref[...], bl) + mm(rl_ref[...], bh)
            back = jnp.concatenate(
                [
                    jnp.concatenate([back[:DET, :DET], back[DET:, :DET]], axis=1),
                    jnp.concatenate([back[:DET, DET:], back[DET:, DET:]], axis=1),
                ],
                axis=0,
            )
            zh, zl = split(back)
            change = mm(zh, lh_ref[...]) + mm(zl, lh_ref[...]) + mm(zh, ll_ref[...])
            for i in range(2):
                k = 2 * j + i
                cr, ci = change[i * DET : i * DET + DET, :DET], change[i * DET : i * DET + DET, DET:]
                pr, pi = probe_ref[k, 0], probe_ref[k, 1]
                ar, ai = patch_ref[0], patch_ref[1]
                sums_ref[2 * k] += ar * cr + ai * ci
                sums_ref[2 * k + 1] += ar * ci - ai * cr
                num_ref[0] += pr * cr + pi * ci
                num_ref[1] += pr * ci - pi * cr
        ar, ai = patch_ref[0], patch_ref[1]
        sums_ref[2 * modes] += ar * ar + ai * ai
        sums_ref[2 * modes + 1] += patterns_ref[position]
        for c in range(3):
            value = num_ref[c] if c < 2 else power
            value = jnp.concatenate([value, jnp.zeros((8, DET), jnp.float32)], axis=0)
            value = pltpu.roll(value, drop, 0)
            value = jnp.concatenate([value, jnp.zeros_like(value)], axis=1)
            frame_ref[c, pl.ds(slab, TALL), pl.ds(tile, 2 * DET)] += pltpu.roll(value, shift, 1)
        return 0

    lax.fori_loop(0, patterns_ref.shape[0], one_position, 0)


def positions(local, probe, patterns, extended):
    modes = probe.shape[0]
    return pl.pallas_call(
        positions_kernel,
        out_shape=(
            jax.ShapeDtypeStruct((2 * modes + 2, DET, DET), jnp.float32),
            jax.ShapeDtypeStruct((3,) + extended.shape[1:], jnp.float32),
        ),
        in_specs=[SMEM] + [VMEM] * 7,
        out_specs=(VMEM, VMEM),
        scratch_shapes=[
            pltpu.VMEM((2, DET, DET), jnp.float32),
            pltpu.VMEM((modes // 2, 2 * DET, 2 * DET), jnp.float32),
            pltpu.VMEM((2, DET, DET), jnp.float32),
        ],
        name="positions",
    )(local, probe, patterns, extended, *split_tables())


def extended_2(array, sides, width):
    for axis, dim in sides:
        size, length = (lax.axis_size(axis), array.shape[dim])
        up = [(i, (i + 1) % size) for i in range(size - 1)]
        down = [(j, i) for i, j in up]
        last = lax.slice_in_dim(array, length - width, length, axis=dim)
        first = lax.slice_in_dim(array, 0, width, axis=dim)
        before = lax.ppermute(last, axis, up)
        after = lax.ppermute(first, axis, down)
        array = jnp.concatenate([before, array, after], axis=dim)
    return array


def newton_steps(gram_re, gram_im):
    mode_count = gram_re.shape[0]
    upper = jnp.concatenate([gram_re, -gram_im], axis=1)
    lower = jnp.concatenate([gram_im, gram_re], axis=1)
    embedded = jnp.concatenate([upper, lower], axis=0)
    frobenius = jnp.sqrt(jnp.sum(embedded * embedded))
    identity = jnp.eye(2 * mode_count, dtype=jnp.float32)
    current = embedded / frobenius
    inverse = identity
    for repeat in range(NS_STEPS):
        factor = 1.5 * identity - 0.5 * jnp.dot(
            inverse, current, precision=highest, preferred_element_type=jnp.float32
        )
        current = jnp.dot(current, factor, precision=highest, preferred_element_type=jnp.float32)
        inverse = jnp.dot(factor, inverse, precision=highest, preferred_element_type=jnp.float32)
    inverse = inverse / jnp.sqrt(frobenius)
    return (inverse[:mode_count, :mode_count], inverse[mode_count:, :mode_count])


def gram_parts(mode_rows):
    real_rows = mode_rows[0::2]
    imag_rows = mode_rows[1::2]
    gram_re = jnp.dot(
        real_rows, real_rows.T, precision=highest, preferred_element_type=jnp.float32
    ) + jnp.dot(imag_rows, imag_rows.T, precision=highest, preferred_element_type=jnp.float32)
    gram_im = jnp.dot(
        real_rows, imag_rows.T, precision=highest, preferred_element_type=jnp.float32
    ) - jnp.dot(imag_rows, real_rows.T, precision=highest, preferred_element_type=jnp.float32)
    return (gram_re, gram_im)


def orthonormal_rows(mode_rows, gram_re, gram_im, power_ratio):
    real_rows = mode_rows[0::2]
    imag_rows = mode_rows[1::2]
    mix_re, mix_im = newton_steps(gram_re, gram_im)
    ortho_re = jnp.dot(
        mix_re.T, real_rows, precision=highest, preferred_element_type=jnp.float32
    ) - jnp.dot(mix_im.T, imag_rows, precision=highest, preferred_element_type=jnp.float32)
    ortho_im = jnp.dot(
        mix_im.T, real_rows, precision=highest, preferred_element_type=jnp.float32
    ) + jnp.dot(mix_re.T, imag_rows, precision=highest, preferred_element_type=jnp.float32)
    weight = jnp.sqrt(power_ratio * jnp.diagonal(gram_re))
    joined = jnp.stack([ortho_re, ortho_im], axis=1) * weight[:, None, None]
    return joined.reshape(mode_rows.shape)


def fold_interior(frame_sum, folded, detector, block_rows, block_cols):
    rows_end = block_rows + 3 * detector
    cols_end = block_cols + 3 * detector
    centre_rows = slice(2 * detector, 2 * detector + block_rows)
    centre_cols = slice(2 * detector, 2 * detector + block_cols)
    interior = frame_sum[:, detector : detector + block_rows, detector : detector + block_cols]
    interior = interior.at[:, :detector, :].add(folded[:, :detector, centre_cols])
    interior = interior.at[:, block_rows - detector :, :].add(folded[:, rows_end:, centre_cols])
    interior = interior.at[:, :, :detector].add(folded[:, centre_rows, :detector])
    interior = interior.at[:, :, block_cols - detector :].add(folded[:, centre_rows, cols_end:])
    interior = interior.at[:, :detector, :detector].add(folded[:, :detector, :detector])
    interior = interior.at[:, :detector, block_cols - detector :].add(
        folded[:, :detector, cols_end:]
    )
    interior = interior.at[:, block_rows - detector :, :detector].add(
        folded[:, rows_end:, :detector]
    )
    interior = interior.at[:, block_rows - detector :, block_cols - detector :].add(
        folded[:, rows_end:, cols_end:]
    )
    return interior


def body(probe_modes, patterns, specimen, offsets):
    mode_count = probe_modes.shape[0]
    block_rows, block_cols = specimen.shape[1:]
    sides = (("scan", 1), ("tile", 2))
    extended = extended_2(specimen, sides, DET)
    base = jnp.stack(
        [
            lax.axis_index("scan") * block_rows - DET,
            lax.axis_index("tile") * block_cols - DET,
        ]
    )
    sums, frame_sum = positions(offsets - base, probe_modes, patterns, extended)
    folded = extended_2(frame_sum, sides, DET)
    interior = fold_interior(frame_sum, folded, DET, block_rows, block_cols)
    new_specimen = specimen + interior[0:2] / (interior[2] + OBJECT_REG)[None]
    totals = lax.psum(sums.reshape(2 * mode_count + 2, -1), ("scan", "tile"))
    probe_rows = probe_modes.reshape(2 * mode_count, -1)
    light = totals[2 * mode_count : 2 * mode_count + 1]
    updated = probe_rows + totals[: 2 * mode_count] / (light + PROBE_REG)
    power = jnp.sum(probe_rows * probe_rows, axis=0)
    power_ratio = jnp.sum(totals[2 * mode_count + 1]) / (jnp.sum(power * light[0]) + TOTAL_EPS)
    gram_re, gram_im = gram_parts(updated)
    new_probe = orthonormal_rows(updated, gram_re, gram_im, power_ratio).reshape(probe_modes.shape)
    return (new_probe, new_specimen)


def solution(mesh):
    return jax.shard_map(
        body,
        mesh=mesh,
        in_specs=(
            P(),
            P(("scan", "tile"), None, None),
            P(None, "scan", "tile"),
            P(("scan", "tile"), None),
        ),
        out_specs=(P(), P(None, "scan", "tile")),
        check_vma=False,
    )
```

```python
import math

import jax
import jax.numpy as jnp
import ml_dtypes
import numpy as np
from jax import lax
from jax.experimental import pallas as pl
from jax.experimental.pallas import tpu as pltpu
from jax.sharding import PartitionSpec as P

NS_STEPS = 8
DET = 128
TALL = 136
LIGHT_FLOOR = 0.05
OBJECT_REG = 0.5
PROBE_REG = 1.0
TOTAL_EPS = 1e-06
VMEM = pl.BlockSpec(memory_space=pltpu.VMEM)
SMEM = pl.BlockSpec(memory_space=pltpu.SMEM)
highest = lax.Precision.HIGHEST


def split_tables():
    index = np.arange(DET)
    angles = -2.0 * math.pi / DET * (index[:, None] * index[None, :] % DET)
    cos, sin = np.cos(angles) / math.sqrt(DET), np.sin(angles) / math.sqrt(DET)
    right = np.block([[cos, sin], [-sin, cos]])
    tables = []
    for matrix in (right, right.T):
        high = matrix.astype(ml_dtypes.bfloat16)
        low = (matrix - high.astype(np.float64)).astype(ml_dtypes.bfloat16)
        tables += [high, low]
    return [jnp.asarray(table) for table in tables]


def split(value):
    high = value.astype(jnp.bfloat16)
    return high, (value - high.astype(jnp.float32)).astype(jnp.bfloat16)


def mm(a, b):
    return jnp.dot(a, b, preferred_element_type=jnp.float32)


def place(channel, modes):
    return channel + channel // modes


def window_of(local_ref, position):
    row = local_ref[position, 0]
    col = local_ref[position, 1]
    tile = jnp.minimum(col // DET, 2)
    slab = jnp.minimum(row // 8, 31)
    return pl.multiple_of(slab * 8, 8), row - slab * 8, pl.multiple_of(tile * DET, DET), col - tile * DET


def positions_kernel(
    local_ref,
    probe_ref,
    patterns_ref,
    ext_ref,
    rh_ref,
    rl_ref,
    lh_ref,
    ll_ref,
    sums_ref,
    frame_ref,
    patch_ref,
    far_ref,
    num_ref,
):
    modes = probe_ref.shape[0]
    pairs = modes // 2
    power = jnp.zeros((DET, DET), jnp.float32)
    for k in range(modes):
        power = power + probe_ref[k, 0] * probe_ref[k, 0] + probe_ref[k, 1] * probe_ref[k, 1]
    sums_ref[...] = jnp.zeros_like(sums_ref)
    frame_ref[...] = jnp.zeros_like(frame_ref)

    def one_position(position, _):
        slab, drop, tile, shift = window_of(local_ref, position)
        for c in range(2):
            window = ext_ref[c, pl.ds(slab, TALL), pl.ds(tile, 2 * DET)]
            window = pltpu.roll(window, lax.rem(2 * DET - shift, 2 * DET), 1)[:, :DET]
            patch_ref[c] = pltpu.roll(window, lax.rem(TALL - drop, TALL), 0)[:DET]
        model = jnp.zeros((DET, DET), jnp.float32)
        for j in range(pairs):
            lefts = []
            for k in (2 * j, 2 * j + 1):
                pr, pi = probe_ref[k, 0], probe_ref[k, 1]
                ar, ai = patch_ref[0], patch_ref[1]
                lefts.append(jnp.concatenate([pr * ar - pi * ai, pr * ai + pi * ar], axis=1))
            xh, xl = split(jnp.concatenate(lefts, axis=0))
            half = mm(xh, rh_ref[...]) + mm(xl, rh_ref[...]) + mm(xh, rl_ref[...])
            half = jnp.concatenate(
                [
                    jnp.concatenate([half[:DET, :DET], half[DET:, :DET]], axis=1),
                    jnp.concatenate([half[:DET, DET:], half[DET:, DET:]], axis=1),
                ],
                axis=0,
            )
            yh, yl = split(half)
            far = mm(lh_ref[...], yh) + mm(lh_ref[...], yl) + mm(ll_ref[...], yh)
            far_ref[j] = far
            squares = far * far
            squares = squares[:DET] + squares[DET:]
            model = model + squares[:, :DET] + squares[:, DET:]
        factor = jnp.sqrt(patterns_ref[position]) / jnp.sqrt(jnp.maximum(model, LIGHT_FLOOR)) - 1.0
        wide = jnp.concatenate([factor, factor], axis=1)
        wide = jnp.concatenate([wide, wide], axis=0)
        num_ref[...] = jnp.zeros_like(num_ref)
        for j in range(pairs):
            bh, bl = split(far_ref[j] * wide)
            back = mm(rh_ref[...], bh) + mm(rh_ref[...], bl) + mm(rl_ref[...], bh)
            back = jnp.concatenate(
                [
                    jnp.concatenate([back[:DET, :DET], back[DET:, :DET]], axis=1),
                    jnp.concatenate([back[:DET, DET:], back[DET:, DET:]], axis=1),
                ],
                axis=0,
            )
            zh, zl = split(back)
            change = mm(zh, lh_ref[...]) + mm(zl, lh_ref[...]) + mm(zh, ll_ref[...])
            for i in range(2):
                k = 2 * j + i
                cr, ci = change[i * DET : i * DET + DET, :DET], change[i * DET : i * DET + DET, DET:]
                pr, pi = probe_ref[k, 0], probe_ref[k, 1]
                ar, ai = patch_ref[0], patch_ref[1]
                at = place(2 * k, modes)
                sums_ref[at] += ar * cr + ai * ci
                sums_ref[at + 1] += ar * ci - ai * cr
                num_ref[0] += pr * cr + pi * ci
                num_ref[1] += pr * ci - pi * cr
        ar, ai = patch_ref[0], patch_ref[1]
        sums_ref[modes] += ar * ar + ai * ai
        sums_ref[2 * modes + 1] += patterns_ref[position]
        for c in range(3):
            value = num_ref[c] if c < 2 else power
            value = jnp.concatenate([value, jnp.zeros((8, DET), jnp.float32)], axis=0)
            value = pltpu.roll(value, drop, 0)
            value = jnp.concatenate([value, jnp.zeros_like(value)], axis=1)
            frame_ref[c, pl.ds(slab, TALL), pl.ds(tile, 2 * DET)] += pltpu.roll(value, shift, 1)
        return 0

    lax.fori_loop(0, patterns_ref.shape[0], one_position, 0)


def positions(local, probe, patterns, extended):
    modes = probe.shape[0]
    return pl.pallas_call(
        positions_kernel,
        out_shape=(
            jax.ShapeDtypeStruct((2 * modes + 2, DET, DET), jnp.float32),
            jax.ShapeDtypeStruct((3,) + extended.shape[1:], jnp.float32),
        ),
        in_specs=[SMEM] + [VMEM] * 7,
        out_specs=(VMEM, VMEM),
        scratch_shapes=[
            pltpu.VMEM((2, DET, DET), jnp.float32),
            pltpu.VMEM((modes // 2, 2 * DET, 2 * DET), jnp.float32),
            pltpu.VMEM((2, DET, DET), jnp.float32),
        ],
        name="positions",
    )(local, probe, patterns, extended, *split_tables())


def extended_2(array, sides, width):
    for axis, dim in sides:
        size, length = (lax.axis_size(axis), array.shape[dim])
        up = [(i, (i + 1) % size) for i in range(size - 1)]
        down = [(j, i) for i, j in up]
        last = lax.slice_in_dim(array, length - width, length, axis=dim)
        first = lax.slice_in_dim(array, 0, width, axis=dim)
        before = lax.ppermute(last, axis, up)
        after = lax.ppermute(first, axis, down)
        array = jnp.concatenate([before, array, after], axis=dim)
    return array


SPLITS = ((0, 6), (6, 13))
AXES = ("x", "y")
GRID = {"x": 4, "y": 4, "z": 8, "core": 2}


def dot32(a, b, contract=(1, 0)):
    return lax.dot_general(
        a,
        b,
        (((contract[0],), (contract[1],)), ((), ())),
        precision=highest,
        preferred_element_type=jnp.float32,
    )


def my_place():
    scan = lax.axis_index("scan")
    tile = lax.axis_index("tile")
    return {
        "core": lax.rem(scan, 2),
        "z": lax.rem(scan // 2, 8),
        "x": lax.rem(scan // 16, 4),
        "y": (scan // 64) * 2 + tile,
    }


def device_at(place_of):
    high, low = place_of["y"] // 2, lax.rem(place_of["y"], 2)
    return (((high * 4 + place_of["x"]) * 8 + place_of["z"]) * 2 + place_of["core"], low)


def moved(here, axis, step):
    return {**here, axis: lax.rem(here[axis] + step, GRID[axis])}


def reduce_kernel(
    sums_ref,
    probe_ref,
    upd_ref,
    gram_ref,
    held,
    work,
    first_a,
    first_b,
    second_a,
    second_b,
    part,
    third,
    both,
    block,
    grams,
    send_sem,
    recv_sem,
):
    here = my_place()
    x, y, z, core = here["x"], here["y"], here["z"], here["core"]
    partner = moved(here, "core", 1)
    other = partner["core"]
    peers = [moved(here, axis, step) for axis in ("x", "y", "z") for step in range(1, GRID[axis])]
    barrier = pltpu.get_barrier_semaphore()
    for peer in peers + [partner]:
        pl.semaphore_signal(
            barrier, inc=1, device_id=device_at(peer), device_id_type=pl.DeviceIdType.MESH
        )
    pl.semaphore_wait(barrier, len(peers) + 1)
    started = []

    def send(src, dst, peer):
        index = len(started)
        copy = pltpu.make_async_remote_copy(
            src_ref=src,
            dst_ref=dst,
            send_sem=send_sem.at[index],
            recv_sem=recv_sem.at[index],
            device_id=device_at(peer),
            device_id_type=pl.DeviceIdType.MESH,
        )
        copy.start()
        started.append(copy)
        return copy

    def around(axis):
        return [(step, moved(here, axis, step)) for step in range(1, GRID[axis])]

    halves = []
    for low, high in SPLITS:
        rows = pl.ds(low, high - low)
        halves.append(send(sums_ref.at[other, rows], held.at[rows], partner))
    firsts = []
    for half, (low, high) in enumerate(SPLITS):
        halves[half].wait_recv()
        rows = pl.ds(low, high - low)
        work[rows] = sums_ref[core, rows] + held[rows]
        if half == 0:
            firsts.append(
                [send(work.at[rows, p["x"]], first_a.at[i - 1], p) for i, p in around("x")]
            )
        else:
            firsts.append(
                [send(work.at[rows, :, p["y"]], first_b.at[i - 1], p) for i, p in around("y")]
            )
    seconds = []
    rows_a, rows_b = (pl.ds(low, high - low) for low, high in SPLITS)
    for copy in firsts[0]:
        copy.wait_recv()
    work[rows_a, x] += first_a[0] + first_a[1] + first_a[2]
    seconds.append([send(work.at[rows_a, x, p["y"]], second_a.at[i - 1], p) for i, p in around("y")])
    for copy in firsts[1]:
        copy.wait_recv()
    work[rows_b, :, y] += first_b[0] + first_b[1] + first_b[2]
    seconds.append([send(work.at[rows_b, p["x"], y], second_b.at[i - 1], p) for i, p in around("x")])
    for copy in seconds[0]:
        copy.wait_recv()
    part[rows_a] = work[rows_a, x, y] + second_a[0] + second_a[1] + second_a[2]
    for copy in seconds[1]:
        copy.wait_recv()
    part[rows_b] = work[rows_b, x, y] + second_b[0] + second_b[1] + second_b[2]
    part[pl.ds(13, 3)] = jnp.zeros((3, 8, DET), jnp.float32)

    thirds = [
        send(part.at[pl.ds(2 * p["z"], 2)], third.at[i - 1], p) for i, p in around("z")
    ]
    mine = part[pl.ds(2 * z, 2)]
    for i, copy in enumerate(thirds):
        copy.wait_recv()
        mine = mine + third[i]
    pair = pl.ds(2 * z, 2)
    both[core, pair] = mine
    backs = [send(both.at[core, pair], both.at[core, pair], p) for i, p in around("z")]
    for copy in backs:
        copy.wait_recv()
    across = send(both.at[core], both.at[core], partner)
    across.wait_recv()

    light = both[0, 12]
    power = jnp.zeros((8, DET), jnp.float32)
    for channel in range(24):
        old = probe_ref[channel, x, y]
        power = power + old * old
        new = old + both[channel // 12, channel % 12] / (light + PROBE_REG)
        block[channel // 12, pl.ds(8 * (channel % 12), 8)] = new
    for i in range(12):
        upd_ref[core, i, x, y] = block[core, pl.ds(8 * i, 8)]
    rows = jnp.concatenate(
        [
            jnp.concatenate([block[c, pl.ds(s, 12, stride=8)] for s in range(8)], axis=1)
            for c in range(2)
        ],
        axis=0,
    )
    padded = jnp.concatenate([rows, jnp.zeros((DET - 24, 8 * DET), jnp.float32)], axis=0)
    line = lax.broadcasted_iota(jnp.int32, (8, DET), 0)
    total = jnp.sum(both[1, 12], axis=0, keepdims=True)
    model = jnp.sum(power * light, axis=0, keepdims=True)
    extra = jnp.where(line == 0, total, jnp.where(line == 1, model, 0.0))
    grams[0, y] = jnp.concatenate([dot32(rows, padded, (1, 1)), extra], axis=0)

    one_a, one_b = pl.ds(0, 6), pl.ds(6, 6)
    gram_y = [send(grams.at[0, y], grams.at[0, y], p) for i, p in around("y")]
    spot_a, spot_b = upd_ref.at[core, one_a, x, y], upd_ref.at[core, one_b, x, y]
    near_a = [send(spot_a, spot_a, p) for i, p in around("y")]
    near_b = [send(spot_b, spot_b, p) for i, p in around("x")]
    for copy in gram_y:
        copy.wait_recv()
    grams[1, x] = (grams[0, 0] + grams[0, 1]) + (grams[0, 2] + grams[0, 3])
    gram_x = [send(grams.at[1, x], grams.at[1, x], p) for i, p in around("x")]
    for copy in near_a:
        copy.wait_recv()
    line_a = upd_ref.at[core, one_a, x]
    far_a = [send(line_a, line_a, p) for i, p in around("x")]
    for copy in near_b:
        copy.wait_recv()
    line_b = upd_ref.at[core, one_b, :, y]
    far_b = [send(line_b, line_b, p) for i, p in around("y")]
    last = [send(line_a, line_a, partner), send(line_b, line_b, partner)]
    for copy in gram_x:
        copy.wait_recv()
    gram_ref[...] = (grams[1, 0] + grams[1, 1]) + (grams[1, 2] + grams[1, 3])
    for step in range(1, 4):
        far_a[step - 1].wait_recv()
        got = upd_ref.at[core, one_a, lax.rem(x + 4 - step, 4)]
        last.append(send(got, got, partner))
        far_b[step - 1].wait_recv()
        got = upd_ref.at[core, one_b, :, lax.rem(y + 4 - step, 4)]
        last.append(send(got, got, partner))
    for copy in last:
        copy.wait_recv()
    for copy in started:
        copy.wait_send()


COPIES = 55


def reduced(sums, probe):
    f32 = jnp.float32
    return pl.pallas_call(
        reduce_kernel,
        out_shape=(
            jax.ShapeDtypeStruct((2, 12, 4, 4, 8, DET), f32),
            jax.ShapeDtypeStruct((32, DET), f32),
        ),
        in_specs=[VMEM, VMEM],
        out_specs=(VMEM, VMEM),
        scratch_shapes=[
            pltpu.VMEM((13, 4, 4, 8, DET), f32),
            pltpu.VMEM((13, 4, 4, 8, DET), f32),
            pltpu.VMEM((3, 6, 4, 8, DET), f32),
            pltpu.VMEM((3, 7, 4, 8, DET), f32),
            pltpu.VMEM((3, 6, 8, DET), f32),
            pltpu.VMEM((3, 7, 8, DET), f32),
            pltpu.VMEM((16, 8, DET), f32),
            pltpu.VMEM((7, 2, 8, DET), f32),
            pltpu.VMEM((2, 16, 8, DET), f32),
            pltpu.VMEM((2, 96, DET), f32),
            pltpu.VMEM((2, 4, 32, DET), f32),
            pltpu.SemaphoreType.DMA((COPIES,)),
            pltpu.SemaphoreType.DMA((COPIES,)),
        ],
        compiler_params=pltpu.CompilerParams(collective_id=0, has_side_effects=True),
        name="reduce_all",
    )(sums.reshape(2, 13, 4, 4, 8, DET), probe.reshape(24, 4, 4, 8, DET))


def mixing(gram):
    size = 24
    row = lax.broadcasted_iota(jnp.int32, (size, size), 0)
    col = lax.broadcasted_iota(jnp.int32, (size, size), 1)
    identity = jnp.where(row == col, 1.0, 0.0)
    even = lax.rem(row, 2) == 0
    turn = jnp.where(even & (col == row + 1), -1.0, jnp.where(~even & (col == row - 1), 1.0, 0.0))
    products = gram[:size, :size]
    embedded = products + dot32(dot32(turn, products), turn, (1, 1))
    frobenius = jnp.sqrt(jnp.sum(embedded * embedded, keepdims=True))
    current = embedded / frobenius
    inverse = identity
    for repeat in range(NS_STEPS):
        factor = 1.5 * identity - 0.5 * dot32(inverse, current)
        current = dot32(current, factor)
        inverse = dot32(factor, inverse)
    total = jnp.sum(gram[size : size + 1], keepdims=True)
    model = jnp.sum(gram[size + 1 : size + 2], keepdims=True)
    ratio = total / (model + TOTAL_EPS)
    diagonal = jnp.sum(embedded * identity, axis=1, keepdims=True)
    return inverse / jnp.sqrt(frobenius) * jnp.sqrt(ratio * diagonal)


def ortho_kernel(gram_ref, upd_ref, out_ref):
    mix = mixing(gram_ref[...])
    tall = lax.broadcasted_iota(jnp.int32, (192, 24), 0)
    wide = lax.broadcasted_iota(jnp.int32, (192, 24), 1)
    expand = jnp.where(tall // 8 == wide, 1.0, 0.0)
    large = dot32(dot32(expand, mix), expand, (1, 1))
    row = lax.broadcasted_iota(jnp.int32, (192, 192), 0)
    col = lax.broadcasted_iota(jnp.int32, (192, 192), 1)
    large = jnp.where(lax.rem(row, 8) == lax.rem(col, 8), large, 0.0)
    for b in range(0, 16, 2):
        blocks = [upd_ref[:, b + i].reshape(192, DET) for i in range(2)]
        result = dot32(large, jnp.concatenate(blocks, axis=1))
        for i in range(2):
            out_ref[:, b + i] = result[:, i * DET : i * DET + DET].reshape(24, 8, DET)


def orthonormal(gram, updated):
    return pl.pallas_call(
        ortho_kernel,
        out_shape=jax.ShapeDtypeStruct((24, 16, 8, DET), jnp.float32),
        in_specs=[VMEM, VMEM],
        out_specs=VMEM,
        name="orthonormal",
    )(gram, updated.reshape(24, 16, 8, DET))


def fold_interior(frame_sum, folded, detector, block_rows, block_cols):
    rows_end = block_rows + 3 * detector
    cols_end = block_cols + 3 * detector
    centre_rows = slice(2 * detector, 2 * detector + block_rows)
    centre_cols = slice(2 * detector, 2 * detector + block_cols)
    interior = frame_sum[:, detector : detector + block_rows, detector : detector + block_cols]
    interior = interior.at[:, :detector, :].add(folded[:, :detector, centre_cols])
    interior = interior.at[:, block_rows - detector :, :].add(folded[:, rows_end:, centre_cols])
    interior = interior.at[:, :, :detector].add(folded[:, centre_rows, :detector])
    interior = interior.at[:, :, block_cols - detector :].add(folded[:, centre_rows, cols_end:])
    interior = interior.at[:, :detector, :detector].add(folded[:, :detector, :detector])
    interior = interior.at[:, :detector, block_cols - detector :].add(
        folded[:, :detector, cols_end:]
    )
    interior = interior.at[:, block_rows - detector :, :detector].add(
        folded[:, rows_end:, :detector]
    )
    interior = interior.at[:, block_rows - detector :, block_cols - detector :].add(
        folded[:, rows_end:, cols_end:]
    )
    return interior


def body(probe_modes, patterns, specimen, offsets):
    block_rows, block_cols = specimen.shape[1:]
    sides = (("scan", 1), ("tile", 2))
    extended = extended_2(specimen, sides, DET)
    base = jnp.stack(
        [
            lax.axis_index("scan") * block_rows - DET,
            lax.axis_index("tile") * block_cols - DET,
        ]
    )
    sums, frame_sum = positions(offsets - base, probe_modes, patterns, extended)
    folded = extended_2(frame_sum, sides, DET)
    interior = fold_interior(frame_sum, folded, DET, block_rows, block_cols)
    new_specimen = specimen + interior[0:2] / (interior[2] + OBJECT_REG)[None]
    updated, gram = reduced(sums, probe_modes)
    new_probe = orthonormal(gram, updated).reshape(probe_modes.shape)
    return (new_probe, new_specimen)


def solution(mesh):
    return jax.shard_map(
        body,
        mesh=mesh,
        in_specs=(
            P(),
            P(("scan", "tile"), None, None),
            P(None, "scan", "tile"),
            P(("scan", "tile"), None),
        ),
        out_specs=(P(), P(None, "scan", "tile")),
        check_vma=False,
    )
```

```python
import math

import jax
import jax.numpy as jnp
import ml_dtypes
import numpy as np
from jax import lax
from jax.experimental import pallas as pl
from jax.experimental.pallas import tpu as pltpu
from jax.sharding import PartitionSpec as P

NS_STEPS = 8
DET = 128
TALL = 136
LIGHT_FLOOR = 0.05
OBJECT_REG = 0.5
PROBE_REG = 1.0
TOTAL_EPS = 1e-06
VMEM = pl.BlockSpec(memory_space=pltpu.VMEM)
SMEM = pl.BlockSpec(memory_space=pltpu.SMEM)
highest = lax.Precision.HIGHEST


def split_tables():
    index = np.arange(DET)
    angles = -2.0 * math.pi / DET * (index[:, None] * index[None, :] % DET)
    cos, sin = np.cos(angles) / math.sqrt(DET), np.sin(angles) / math.sqrt(DET)
    right = np.block([[cos, sin], [-sin, cos]])
    tables = []
    for matrix in (right, right.T):
        high = matrix.astype(ml_dtypes.bfloat16)
        low = (matrix - high.astype(np.float64)).astype(ml_dtypes.bfloat16)
        tables += [high, low]
    return [jnp.asarray(table) for table in tables]


def split(value):
    high = value.astype(jnp.bfloat16)
    return high, (value - high.astype(jnp.float32)).astype(jnp.bfloat16)


def mm(a, b):
    return jnp.dot(a, b, preferred_element_type=jnp.float32)


def place(channel, modes):
    return channel + channel // modes


def window_of(local_ref, position):
    row = local_ref[position, 0] - (lax.axis_index("scan") - 1) * DET
    col = local_ref[position, 1] - (2 * lax.axis_index("tile") - 1) * DET
    tile = jnp.minimum(col // DET, 2)
    slab = jnp.minimum(row // 8, 31)
    return pl.multiple_of(slab * 8, 8), row - slab * 8, pl.multiple_of(tile * DET, DET), col - tile * DET


def positions_kernel(
    local_ref,
    probe_ref,
    patterns_ref,
    ext_ref,
    rh_ref,
    rl_ref,
    lh_ref,
    ll_ref,
    sums_ref,
    frame_ref,
    patch_ref,
    far_ref,
    num_ref,
):
    modes = probe_ref.shape[0]
    pairs = modes // 2
    power = jnp.zeros((DET, DET), jnp.float32)
    for k in range(modes):
        power = power + probe_ref[k, 0] * probe_ref[k, 0] + probe_ref[k, 1] * probe_ref[k, 1]
    sums_ref[...] = jnp.zeros_like(sums_ref)
    frame_ref[...] = jnp.zeros_like(frame_ref)

    def one_position(position, _):
        slab, drop, tile, shift = window_of(local_ref, position)
        for c in range(2):
            window = ext_ref[c, pl.ds(slab, TALL), pl.ds(tile, 2 * DET)]
            window = pltpu.roll(window, lax.rem(2 * DET - shift, 2 * DET), 1)[:, :DET]
            patch_ref[c] = pltpu.roll(window, lax.rem(TALL - drop, TALL), 0)[:DET]
        model = jnp.zeros((DET, DET), jnp.float32)
        for j in range(pairs):
            lefts = []
            for k in (2 * j, 2 * j + 1):
                pr, pi = probe_ref[k, 0], probe_ref[k, 1]
                ar, ai = patch_ref[0], patch_ref[1]
                lefts.append(jnp.concatenate([pr * ar - pi * ai, pr * ai + pi * ar], axis=1))
            xh, xl = split(jnp.concatenate(lefts, axis=0))
            half = mm(xh, rh_ref[...]) + mm(xl, rh_ref[...]) + mm(xh, rl_ref[...])
            half = jnp.concatenate(
                [
                    jnp.concatenate([half[:DET, :DET], half[DET:, :DET]], axis=1),
                    jnp.concatenate([half[:DET, DET:], half[DET:, DET:]], axis=1),
                ],
                axis=0,
            )
            yh, yl = split(half)
            far = mm(lh_ref[...], yh) + mm(lh_ref[...], yl) + mm(ll_ref[...], yh)
            far_ref[j] = far
            squares = far * far
            squares = squares[:DET] + squares[DET:]
            model = model + squares[:, :DET] + squares[:, DET:]
        factor = jnp.sqrt(patterns_ref[position]) / jnp.sqrt(jnp.maximum(model, LIGHT_FLOOR)) - 1.0
        wide = jnp.concatenate([factor, factor], axis=1)
        wide = jnp.concatenate([wide, wide], axis=0)
        num_ref[...] = jnp.zeros_like(num_ref)
        for j in range(pairs):
            bh, bl = split(far_ref[j] * wide)
            back = mm(rh_ref[...], bh) + mm(rh_ref[...], bl) + mm(rl_ref[...], bh)
            back = jnp.concatenate(
                [
                    jnp.concatenate([back[:DET, :DET], back[DET:, :DET]], axis=1),
                    jnp.concatenate([back[:DET, DET:], back[DET:, DET:]], axis=1),
                ],
                axis=0,
            )
            zh, zl = split(back)
            change = mm(zh, lh_ref[...]) + mm(zl, lh_ref[...]) + mm(zh, ll_ref[...])
            for i in range(2):
                k = 2 * j + i
                cr, ci = change[i * DET : i * DET + DET, :DET], change[i * DET : i * DET + DET, DET:]
                pr, pi = probe_ref[k, 0], probe_ref[k, 1]
                ar, ai = patch_ref[0], patch_ref[1]
                at = place(2 * k, modes)
                sums_ref[at] += ar * cr + ai * ci
                sums_ref[at + 1] += ar * ci - ai * cr
                num_ref[0] += pr * cr + pi * ci
                num_ref[1] += pr * ci - pi * cr
        ar, ai = patch_ref[0], patch_ref[1]
        sums_ref[modes] += ar * ar + ai * ai
        sums_ref[2 * modes + 1] += patterns_ref[position]
        for c in range(3):
            value = num_ref[c] if c < 2 else power
            value = jnp.concatenate([value, jnp.zeros((8, DET), jnp.float32)], axis=0)
            value = pltpu.roll(value, drop, 0)
            value = jnp.concatenate([value, jnp.zeros_like(value)], axis=1)
            frame_ref[c, pl.ds(slab, TALL), pl.ds(tile, 2 * DET)] += pltpu.roll(value, shift, 1)
        return 0

    lax.fori_loop(0, patterns_ref.shape[0], one_position, 0)


def positions(local, probe, patterns, extended):
    modes = probe.shape[0]
    return pl.pallas_call(
        positions_kernel,
        out_shape=(
            jax.ShapeDtypeStruct((2 * modes + 2, DET, DET), jnp.float32),
            jax.ShapeDtypeStruct((3,) + extended.shape[1:], jnp.float32),
        ),
        in_specs=[SMEM] + [VMEM] * 7,
        out_specs=(VMEM, VMEM),
        scratch_shapes=[
            pltpu.VMEM((2, DET, DET), jnp.float32),
            pltpu.VMEM((modes // 2, 2 * DET, 2 * DET), jnp.float32),
            pltpu.VMEM((2, DET, DET), jnp.float32),
        ],
        name="positions",
    )(local, probe, patterns, extended, *split_tables())


def signal_all(peers):
    barrier = pltpu.get_barrier_semaphore()
    for peer in peers:
        pl.semaphore_signal(barrier, inc=1, device_id=peer, device_id_type=pl.DeviceIdType.MESH)
    pl.semaphore_wait(barrier, len(peers))


class Copies:
    def __init__(self, send_sem, recv_sem):
        self.send_sem, self.recv_sem, self.started = send_sem, recv_sem, []

    def send(self, src, dst, device):
        index = len(self.started)
        copy = pltpu.make_async_remote_copy(
            src_ref=src,
            dst_ref=dst,
            send_sem=self.send_sem.at[index],
            recv_sem=self.recv_sem.at[index],
            device_id=device,
            device_id_type=pl.DeviceIdType.MESH,
        )
        copy.start()
        self.started.append(copy)
        return copy

    def finish(self):
        for copy in self.started:
            copy.wait_send()


def neighbours():
    scan, tile = lax.axis_index("scan"), lax.axis_index("tile")
    size = lax.axis_size("scan")
    up = (lax.rem(scan + size - 1, size), tile)
    down = (lax.rem(scan + 1, size), tile)
    return up, down, (scan, 1 - tile)


def halo_kernel(spec_ref, ext_ref, send_sem, recv_sem):
    scan, tile = lax.axis_index("scan"), lax.axis_index("tile")
    up, down, across = neighbours()
    signal_all([up, down, across])
    copies = Copies(send_sem, recv_sem)
    own, above, below = pl.ds(DET, DET), pl.ds(0, DET), pl.ds(2 * DET, DET)
    middle = pl.ds(DET, 2 * DET)
    given = pl.ds(pl.multiple_of((1 - tile) * DET, DET), DET)
    empty = pl.ds(pl.multiple_of(tile * 3 * DET, DET), DET)
    filled = pl.ds(pl.multiple_of((1 - tile) * 3 * DET, DET), DET)
    side = copies.send(spec_ref.at[:, :, given], ext_ref.at[:, own, empty], across)
    rest = [
        copies.send(spec_ref, ext_ref.at[:, below, middle], up),
        copies.send(spec_ref, ext_ref.at[:, above, middle], down),
    ]
    ext_ref[:, own, middle] = spec_ref[...]
    ext_ref[:, :, empty] = jnp.zeros((2, 3 * DET, DET), jnp.float32)
    side.wait_recv()
    corner = ext_ref.at[:, own, filled]
    rest.append(copies.send(corner, ext_ref.at[:, below, filled], up))
    rest.append(copies.send(corner, ext_ref.at[:, above, filled], down))
    for copy in rest:
        copy.wait_recv()

    @pl.when(scan == 0)
    def _():
        ext_ref[:, above] = jnp.zeros((2, DET, 4 * DET), jnp.float32)

    @pl.when(scan == lax.axis_size("scan") - 1)
    def _():
        ext_ref[:, below] = jnp.zeros((2, DET, 4 * DET), jnp.float32)

    copies.finish()


def extended_of(specimen):
    return pl.pallas_call(
        halo_kernel,
        out_shape=jax.ShapeDtypeStruct((2, 3 * DET, 4 * DET), jnp.float32),
        in_specs=[VMEM],
        out_specs=VMEM,
        scratch_shapes=[pltpu.SemaphoreType.DMA((5,)), pltpu.SemaphoreType.DMA((5,))],
        compiler_params=pltpu.CompilerParams(collective_id=1, has_side_effects=True),
        name="halo",
    )(specimen)


SPLITS = ((0, 6), (6, 13))
AXES = ("x", "y")
GRID = {"x": 4, "y": 4, "z": 8, "core": 2}


def dot32(a, b, contract=(1, 0)):
    return lax.dot_general(
        a,
        b,
        (((contract[0],), (contract[1],)), ((), ())),
        precision=highest,
        preferred_element_type=jnp.float32,
    )


def my_place():
    scan = lax.axis_index("scan")
    tile = lax.axis_index("tile")
    return {
        "core": lax.rem(scan, 2),
        "z": lax.rem(scan // 2, 8),
        "x": lax.rem(scan // 16, 4),
        "y": (scan // 64) * 2 + tile,
    }


def device_at(place_of):
    high, low = place_of["y"] // 2, lax.rem(place_of["y"], 2)
    return (((high * 4 + place_of["x"]) * 8 + place_of["z"]) * 2 + place_of["core"], low)


def moved(here, axis, step):
    return {**here, axis: lax.rem(here[axis] + step, GRID[axis])}


def reduce_kernel(
    sums_ref,
    probe_ref,
    frame_ref,
    spec_ref,
    upd_ref,
    mix_ref,
    new_ref,
    held,
    work,
    first_a,
    first_b,
    second_a,
    second_b,
    part,
    third,
    both,
    block,
    grams,
    rows_in,
    frame,
    cols_in,
    send_sem,
    recv_sem,
):
    here = my_place()
    x, y, z, core = here["x"], here["y"], here["z"], here["core"]
    partner = moved(here, "core", 1)
    other = partner["core"]
    scan, tile = lax.axis_index("scan"), lax.axis_index("tile")
    up, down, across_tile = neighbours()
    peers = [moved(here, axis, step) for axis in ("x", "y", "z") for step in range(1, GRID[axis])]
    signal_all([device_at(peer) for peer in peers + [partner]] + [up, down])
    copies = Copies(send_sem, recv_sem)

    def send(src, dst, peer):
        return copies.send(src, dst, device_at(peer))

    def around(axis):
        return [(step, moved(here, axis, step)) for step in range(1, GRID[axis])]

    halves = []
    for low, high in SPLITS:
        rows = pl.ds(low, high - low)
        halves.append(send(sums_ref.at[other, rows], held.at[rows], partner))
    span = pl.ds(pl.multiple_of((1 - tile) * DET, DET), 3 * DET)
    from_below = copies.send(frame_ref.at[:, pl.ds(0, DET), span], rows_in.at[0], up)
    from_above = copies.send(frame_ref.at[:, pl.ds(2 * DET, DET), span], rows_in.at[1], down)
    firsts = []
    for half, (low, high) in enumerate(SPLITS):
        halves[half].wait_recv()
        rows = pl.ds(low, high - low)
        work[rows] = sums_ref[core, rows] + held[rows]
        if half == 0:
            firsts.append(
                [send(work.at[rows, p["x"]], first_a.at[i - 1], p) for i, p in around("x")]
            )
        else:
            firsts.append(
                [send(work.at[rows, :, p["y"]], first_b.at[i - 1], p) for i, p in around("y")]
            )
    seconds = []
    rows_a, rows_b = (pl.ds(low, high - low) for low, high in SPLITS)
    for copy in firsts[0]:
        copy.wait_recv()
    work[rows_a, x] += first_a[0] + first_a[1] + first_a[2]
    seconds.append([send(work.at[rows_a, x, p["y"]], second_a.at[i - 1], p) for i, p in around("y")])
    for copy in firsts[1]:
        copy.wait_recv()
    work[rows_b, :, y] += first_b[0] + first_b[1] + first_b[2]
    seconds.append([send(work.at[rows_b, p["x"], y], second_b.at[i - 1], p) for i, p in around("x")])
    for copy in seconds[0]:
        copy.wait_recv()
    part[rows_a] = work[rows_a, x, y] + second_a[0] + second_a[1] + second_a[2]
    for copy in seconds[1]:
        copy.wait_recv()
    part[rows_b] = work[rows_b, x, y] + second_b[0] + second_b[1] + second_b[2]
    part[pl.ds(13, 3)] = jnp.zeros((3, 8, DET), jnp.float32)

    thirds = [
        send(part.at[pl.ds(2 * p["z"], 2)], third.at[i - 1], p) for i, p in around("z")
    ]
    from_below.wait_recv()
    from_above.wait_recv()
    last_row = lax.axis_size("scan") - 1
    for c in range(3):
        added = jnp.where(scan == last_row, 0.0, rows_in[0, c])
        added = added + jnp.where(scan == 0, 0.0, rows_in[1, c])
        frame[c] = frame_ref[c, pl.ds(DET, DET), span] + added
    beyond = pl.ds(pl.multiple_of((1 - tile) * 2 * DET, DET), DET)
    sides = copies.send(frame.at[:, :, beyond], cols_in, across_tile)
    mine = part[pl.ds(2 * z, 2)]
    for i, copy in enumerate(thirds):
        copy.wait_recv()
        mine = mine + third[i]
    pair = pl.ds(2 * z, 2)
    both[core, pair] = mine
    backs = [send(both.at[core, pair], both.at[core, pair], p) for i, p in around("z")]
    for copy in backs:
        copy.wait_recv()
    across = send(both.at[core], both.at[core], partner)
    across.wait_recv()

    light = both[0, 12]
    power = jnp.zeros((8, DET), jnp.float32)
    for channel in range(24):
        old = probe_ref[channel, x, y]
        power = power + old * old
        new = old + both[channel // 12, channel % 12] / (light + PROBE_REG)
        block[channel // 12, pl.ds(8 * (channel % 12), 8)] = new
    for i in range(12):
        upd_ref[core, i, x, y] = block[core, pl.ds(8 * i, 8)]
    rows = jnp.concatenate(
        [
            jnp.concatenate([block[c, pl.ds(s, 12, stride=8)] for s in range(8)], axis=1)
            for c in range(2)
        ],
        axis=0,
    )
    padded = jnp.concatenate([rows, jnp.zeros((DET - 24, 8 * DET), jnp.float32)], axis=0)
    line = lax.broadcasted_iota(jnp.int32, (8, DET), 0)
    total = jnp.sum(both[1, 12], axis=0, keepdims=True)
    model = jnp.sum(power * light, axis=0, keepdims=True)
    extra = jnp.where(line == 0, total, jnp.where(line == 1, model, 0.0))
    grams[0, y] = jnp.concatenate([dot32(rows, padded, (1, 1)), extra], axis=0)

    one_a, one_b = pl.ds(0, 6), pl.ds(6, 6)
    gram_y = [send(grams.at[0, y], grams.at[0, y], p) for i, p in around("y")]
    spot_a, spot_b = upd_ref.at[core, one_a, x, y], upd_ref.at[core, one_b, x, y]
    near_a = [send(spot_a, spot_a, p) for i, p in around("y")]
    near_b = [send(spot_b, spot_b, p) for i, p in around("x")]
    for copy in gram_y:
        copy.wait_recv()
    grams[1, x] = (grams[0, 0] + grams[0, 1]) + (grams[0, 2] + grams[0, 3])
    gram_x = [send(grams.at[1, x], grams.at[1, x], p) for i, p in around("x")]
    for copy in near_a:
        copy.wait_recv()
    line_a = upd_ref.at[core, one_a, x]
    far_a = [send(line_a, line_a, p) for i, p in around("x")]
    for copy in near_b:
        copy.wait_recv()
    line_b = upd_ref.at[core, one_b, :, y]
    far_b = [send(line_b, line_b, p) for i, p in around("y")]
    last = [send(line_a, line_a, partner), send(line_b, line_b, partner)]
    for copy in gram_x:
        copy.wait_recv()
    mix_ref[...] = expanded(mixing((grams[1, 0] + grams[1, 1]) + (grams[1, 2] + grams[1, 3])))
    sides.wait_recv()
    inside = [frame[c, :, pl.ds(pl.multiple_of(tile * DET, DET), 2 * DET)] for c in range(3)]
    for c in range(3):
        left = jnp.where(tile == 1, cols_in[c], 0.0)
        right = jnp.where(tile == 0, cols_in[c], 0.0)
        inside[c] = inside[c] + jnp.concatenate([left, right], axis=1)
    for c in range(2):
        new_ref[c] = spec_ref[c] + inside[c] / (inside[2] + OBJECT_REG)
    for step in range(1, 4):
        far_a[step - 1].wait_recv()
        got = upd_ref.at[core, one_a, lax.rem(x + 4 - step, 4)]
        last.append(send(got, got, partner))
        far_b[step - 1].wait_recv()
        got = upd_ref.at[core, one_b, :, lax.rem(y + 4 - step, 4)]
        last.append(send(got, got, partner))
    for copy in last:
        copy.wait_recv()
    copies.finish()


COPIES = 58


def reduced(sums, probe, frame, specimen):
    f32 = jnp.float32
    return pl.pallas_call(
        reduce_kernel,
        out_shape=(
            jax.ShapeDtypeStruct((2, 12, 4, 4, 8, DET), f32),
            jax.ShapeDtypeStruct((192, 192), f32),
            jax.ShapeDtypeStruct(specimen.shape, f32),
        ),
        in_specs=[VMEM] * 4,
        out_specs=(VMEM,) * 3,
        scratch_shapes=[
            pltpu.VMEM((13, 4, 4, 8, DET), f32),
            pltpu.VMEM((13, 4, 4, 8, DET), f32),
            pltpu.VMEM((3, 6, 4, 8, DET), f32),
            pltpu.VMEM((3, 7, 4, 8, DET), f32),
            pltpu.VMEM((3, 6, 8, DET), f32),
            pltpu.VMEM((3, 7, 8, DET), f32),
            pltpu.VMEM((16, 8, DET), f32),
            pltpu.VMEM((7, 2, 8, DET), f32),
            pltpu.VMEM((2, 16, 8, DET), f32),
            pltpu.VMEM((2, 96, DET), f32),
            pltpu.VMEM((2, 4, 32, DET), f32),
            pltpu.VMEM((2, 3, DET, 3 * DET), f32),
            pltpu.VMEM((3, DET, 3 * DET), f32),
            pltpu.VMEM((3, DET, DET), f32),
            pltpu.SemaphoreType.DMA((COPIES,)),
            pltpu.SemaphoreType.DMA((COPIES,)),
        ],
        compiler_params=pltpu.CompilerParams(collective_id=0, has_side_effects=True),
        name="reduce_all",
    )(sums.reshape(2, 13, 4, 4, 8, DET), probe.reshape(24, 4, 4, 8, DET), frame, specimen)


def mixing(gram):
    size = 24
    row = lax.broadcasted_iota(jnp.int32, (size, size), 0)
    col = lax.broadcasted_iota(jnp.int32, (size, size), 1)
    identity = jnp.where(row == col, 1.0, 0.0)
    even = lax.rem(row, 2) == 0
    turn = jnp.where(even & (col == row + 1), -1.0, jnp.where(~even & (col == row - 1), 1.0, 0.0))
    products = gram[:size, :size]
    embedded = products + dot32(dot32(turn, products), turn, (1, 1))
    frobenius = jnp.sqrt(jnp.sum(embedded * embedded, keepdims=True))
    current = embedded / frobenius
    inverse = identity
    for repeat in range(NS_STEPS):
        factor = 1.5 * identity - 0.5 * dot32(inverse, current)
        current = dot32(current, factor)
        inverse = dot32(factor, inverse)
    total = jnp.sum(gram[size : size + 1], keepdims=True)
    model = jnp.sum(gram[size + 1 : size + 2], keepdims=True)
    ratio = total / (model + TOTAL_EPS)
    diagonal = jnp.sum(embedded * identity, axis=1, keepdims=True)
    return inverse / jnp.sqrt(frobenius) * jnp.sqrt(ratio * diagonal)


def expanded(mix):
    tall = lax.broadcasted_iota(jnp.int32, (192, 24), 0)
    wide = lax.broadcasted_iota(jnp.int32, (192, 24), 1)
    expand = jnp.where(tall // 8 == wide, 1.0, 0.0)
    large = dot32(dot32(expand, mix), expand, (1, 1))
    row = lax.broadcasted_iota(jnp.int32, (192, 192), 0)
    col = lax.broadcasted_iota(jnp.int32, (192, 192), 1)
    return jnp.where(lax.rem(row, 8) == lax.rem(col, 8), large, 0.0)


def ortho_kernel(mix_ref, upd_ref, out_ref):
    large = mix_ref[...]
    for b in range(0, 16, 2):
        blocks = [upd_ref[:, b + i].reshape(192, DET) for i in range(2)]
        result = dot32(large, jnp.concatenate(blocks, axis=1))
        for i in range(2):
            out_ref[:, b + i] = result[:, i * DET : i * DET + DET].reshape(24, 8, DET)


def orthonormal(mix, updated):
    return pl.pallas_call(
        ortho_kernel,
        out_shape=jax.ShapeDtypeStruct((24, 16, 8, DET), jnp.float32),
        in_specs=[VMEM, VMEM],
        out_specs=VMEM,
        name="orthonormal",
    )(mix, updated.reshape(24, 16, 8, DET))


def body(probe_modes, patterns, specimen, offsets):
    extended = extended_of(specimen)
    sums, frame = positions(offsets, probe_modes, patterns, extended)
    updated, mix, new_specimen = reduced(sums, probe_modes, frame, specimen)
    new_probe = orthonormal(mix, updated).reshape(probe_modes.shape)
    return (new_probe, new_specimen)


def solution(mesh):
    return jax.shard_map(
        body,
        mesh=mesh,
        in_specs=(
            P(),
            P(("scan", "tile"), None, None),
            P(None, "scan", "tile"),
            P(("scan", "tile"), None),
        ),
        out_specs=(P(), P(None, "scan", "tile")),
        check_vma=False,
    )
```

```python
import math

import jax
import jax.numpy as jnp
import ml_dtypes
import numpy as np
from jax import lax
from jax.experimental import pallas as pl
from jax.experimental.pallas import tpu as pltpu
from jax.sharding import PartitionSpec as P

NS_STEPS = 8
DET = 128
TALL = 136
LIMIT = 20 * 2**20
LIGHT_FLOOR = 0.05
OBJECT_REG = 0.5
PROBE_REG = 1.0
TOTAL_EPS = 1e-06
VMEM = pl.BlockSpec(memory_space=pltpu.VMEM)
SMEM = pl.BlockSpec(memory_space=pltpu.SMEM)
highest = lax.Precision.HIGHEST


def split_tables():
    index = np.arange(DET)
    angles = -2.0 * math.pi / DET * (index[:, None] * index[None, :] % DET)
    cos, sin = np.cos(angles) / math.sqrt(DET), np.sin(angles) / math.sqrt(DET)
    right = np.block([[cos, sin], [-sin, cos]])
    tables = []
    for matrix in (right, right.T):
        high = matrix.astype(ml_dtypes.bfloat16)
        low = (matrix - high.astype(np.float64)).astype(ml_dtypes.bfloat16)
        tables += [high, low]
    return jnp.asarray(np.stack(tables))


def split(value):
    high = value.astype(jnp.bfloat16)
    return high, (value - high.astype(jnp.float32)).astype(jnp.bfloat16)


def mm(a, b):
    return jnp.dot(a, b, preferred_element_type=jnp.float32)


def place(channel, modes):
    return channel + channel // modes


def window_of(local_ref, position):
    row = local_ref[position, 0] - (lax.axis_index("scan") - 1) * DET
    col = local_ref[position, 1] - (2 * lax.axis_index("tile") - 1) * DET
    tile = jnp.minimum(col // DET, 2)
    slab = jnp.minimum(row // 8, 31)
    return pl.multiple_of(slab * 8, 8), row - slab * 8, pl.multiple_of(tile * DET, DET), col - tile * DET


def positions_kernel(
    local_ref,
    probe_ref,
    patterns_ref,
    ext_ref,
    tables_ref,
    sums_ref,
    frame_ref,
    patch_ref,
    far_ref,
    num_ref,
):
    modes = probe_ref.shape[0]
    pairs = modes // 2
    rh_ref, rl_ref, lh_ref, ll_ref = (tables_ref.at[i] for i in range(4))
    power = jnp.zeros((DET, DET), jnp.float32)
    for k in range(modes):
        power = power + probe_ref[k, 0] * probe_ref[k, 0] + probe_ref[k, 1] * probe_ref[k, 1]
    sums_ref[...] = jnp.zeros_like(sums_ref)
    frame_ref[...] = jnp.zeros_like(frame_ref)

    def one_position(position, _):
        slab, drop, tile, shift = window_of(local_ref, position)
        for c in range(2):
            window = ext_ref[c, pl.ds(slab, TALL), pl.ds(tile, 2 * DET)]
            window = pltpu.roll(window, lax.rem(2 * DET - shift, 2 * DET), 1)[:, :DET]
            patch_ref[c] = pltpu.roll(window, lax.rem(TALL - drop, TALL), 0)[:DET]
        model = jnp.zeros((DET, DET), jnp.float32)
        for j in range(pairs):
            lefts = []
            for k in (2 * j, 2 * j + 1):
                pr, pi = probe_ref[k, 0], probe_ref[k, 1]
                ar, ai = patch_ref[0], patch_ref[1]
                lefts.append(jnp.concatenate([pr * ar - pi * ai, pr * ai + pi * ar], axis=1))
            xh, xl = split(jnp.concatenate(lefts, axis=0))
            half = mm(xh, rh_ref[...]) + mm(xl, rh_ref[...]) + mm(xh, rl_ref[...])
            half = jnp.concatenate(
                [
                    jnp.concatenate([half[:DET, :DET], half[DET:, :DET]], axis=1),
                    jnp.concatenate([half[:DET, DET:], half[DET:, DET:]], axis=1),
                ],
                axis=0,
            )
            yh, yl = split(half)
            far = mm(lh_ref[...], yh) + mm(lh_ref[...], yl) + mm(ll_ref[...], yh)
            far_ref[j] = far
            squares = far * far
            squares = squares[:DET] + squares[DET:]
            model = model + squares[:, :DET] + squares[:, DET:]
        factor = jnp.sqrt(patterns_ref[position]) / jnp.sqrt(jnp.maximum(model, LIGHT_FLOOR)) - 1.0
        wide = jnp.concatenate([factor, factor], axis=1)
        wide = jnp.concatenate([wide, wide], axis=0)
        num_ref[...] = jnp.zeros_like(num_ref)
        for j in range(pairs):
            bh, bl = split(far_ref[j] * wide)
            back = mm(rh_ref[...], bh) + mm(rh_ref[...], bl) + mm(rl_ref[...], bh)
            back = jnp.concatenate(
                [
                    jnp.concatenate([back[:DET, :DET], back[DET:, :DET]], axis=1),
                    jnp.concatenate([back[:DET, DET:], back[DET:, DET:]], axis=1),
                ],
                axis=0,
            )
            zh, zl = split(back)
            change = mm(zh, lh_ref[...]) + mm(zl, lh_ref[...]) + mm(zh, ll_ref[...])
            for i in range(2):
                k = 2 * j + i
                cr, ci = change[i * DET : i * DET + DET, :DET], change[i * DET : i * DET + DET, DET:]
                pr, pi = probe_ref[k, 0], probe_ref[k, 1]
                ar, ai = patch_ref[0], patch_ref[1]
                at = place(2 * k, modes)
                sums_ref[at] += ar * cr + ai * ci
                sums_ref[at + 1] += ar * ci - ai * cr
                num_ref[0] += pr * cr + pi * ci
                num_ref[1] += pr * ci - pi * cr
        ar, ai = patch_ref[0], patch_ref[1]
        sums_ref[modes] += ar * ar + ai * ai
        sums_ref[2 * modes + 1] += patterns_ref[position]
        for c in range(3):
            value = num_ref[c] if c < 2 else power
            value = jnp.concatenate([value, jnp.zeros((8, DET), jnp.float32)], axis=0)
            value = pltpu.roll(value, drop, 0)
            value = jnp.concatenate([value, jnp.zeros_like(value)], axis=1)
            frame_ref[c, pl.ds(slab, TALL), pl.ds(tile, 2 * DET)] += pltpu.roll(value, shift, 1)
        return 0

    lax.fori_loop(0, patterns_ref.shape[0], one_position, 0)


def positions(local, probe, patterns, extended):
    modes = probe.shape[0]
    return pl.pallas_call(
        positions_kernel,
        out_shape=(
            jax.ShapeDtypeStruct((2 * modes + 2, DET, DET), jnp.float32),
            jax.ShapeDtypeStruct((3,) + extended.shape[1:], jnp.float32),
        ),
        in_specs=[SMEM] + [VMEM] * 4,
        out_specs=(VMEM, VMEM),
        scratch_shapes=[
            pltpu.VMEM((2, DET, DET), jnp.float32),
            pltpu.VMEM((modes // 2, 2 * DET, 2 * DET), jnp.float32),
            pltpu.VMEM((2, DET, DET), jnp.float32),
        ],
        compiler_params=pltpu.CompilerParams(vmem_limit_bytes=LIMIT),
        name="positions",
    )(local, probe, patterns, extended, split_tables())


def signal_all(peers):
    barrier = pltpu.get_barrier_semaphore()
    for peer in peers:
        pl.semaphore_signal(barrier, inc=1, device_id=peer, device_id_type=pl.DeviceIdType.MESH)
    pl.semaphore_wait(barrier, len(peers))


class Copies:
    def __init__(self, send_sem, recv_sem):
        self.send_sem, self.recv_sem, self.started = send_sem, recv_sem, []

    def send(self, src, dst, device):
        index = len(self.started)
        copy = pltpu.make_async_remote_copy(
            src_ref=src,
            dst_ref=dst,
            send_sem=self.send_sem.at[index],
            recv_sem=self.recv_sem.at[index],
            device_id=device,
            device_id_type=pl.DeviceIdType.MESH,
        )
        copy.start()
        self.started.append(copy)
        return copy

    def finish(self):
        for copy in self.started:
            copy.wait_send()


def neighbours():
    scan, tile = lax.axis_index("scan"), lax.axis_index("tile")
    size = lax.axis_size("scan")
    up = (lax.rem(scan + size - 1, size), tile)
    down = (lax.rem(scan + 1, size), tile)
    return up, down, (scan, 1 - tile)


def halo_kernel(spec_ref, ext_ref, send_sem, recv_sem):
    scan, tile = lax.axis_index("scan"), lax.axis_index("tile")
    up, down, across = neighbours()
    signal_all([up, down, across])
    copies = Copies(send_sem, recv_sem)
    own, above, below = pl.ds(DET, DET), pl.ds(0, DET), pl.ds(2 * DET, DET)
    middle = pl.ds(DET, 2 * DET)
    given = pl.ds(pl.multiple_of((1 - tile) * DET, DET), DET)
    empty = pl.ds(pl.multiple_of(tile * 3 * DET, DET), DET)
    filled = pl.ds(pl.multiple_of((1 - tile) * 3 * DET, DET), DET)
    pieces = [(c, r * 64) for c in range(2) for r in range(2)]
    side = [
        copies.send(
            spec_ref.at[c, pl.ds(r, 64), given], ext_ref.at[c, pl.ds(DET + r, 64), empty], across
        )
        for c, r in pieces
    ]
    rest = [
        copies.send(spec_ref, ext_ref.at[:, below, middle], up),
        copies.send(spec_ref, ext_ref.at[:, above, middle], down),
    ]
    ext_ref[:, own, middle] = spec_ref[...]
    ext_ref[:, :, empty] = jnp.zeros((2, 3 * DET, DET), jnp.float32)
    for (c, r), copy in zip(pieces, side):
        copy.wait_recv()
        corner = ext_ref.at[c, pl.ds(DET + r, 64), filled]
        rest.append(copies.send(corner, ext_ref.at[c, pl.ds(2 * DET + r, 64), filled], up))
        rest.append(copies.send(corner, ext_ref.at[c, pl.ds(r, 64), filled], down))
    for copy in rest:
        copy.wait_recv()

    @pl.when(scan == 0)
    def _():
        ext_ref[:, above] = jnp.zeros((2, DET, 4 * DET), jnp.float32)

    @pl.when(scan == lax.axis_size("scan") - 1)
    def _():
        ext_ref[:, below] = jnp.zeros((2, DET, 4 * DET), jnp.float32)

    copies.finish()


def extended_of(specimen):
    return pl.pallas_call(
        halo_kernel,
        out_shape=jax.ShapeDtypeStruct((2, 3 * DET, 4 * DET), jnp.float32),
        in_specs=[VMEM],
        out_specs=VMEM,
        scratch_shapes=[pltpu.SemaphoreType.DMA((14,)), pltpu.SemaphoreType.DMA((14,))],
        compiler_params=pltpu.CompilerParams(collective_id=1, has_side_effects=True, vmem_limit_bytes=LIMIT),
        name="halo",
    )(specimen)


SPLITS = ((0, 6), (6, 13))
AXES = ("x", "y")
GRID = {"x": 4, "y": 4, "z": 8, "core": 2}


def dot32(a, b, contract=(1, 0)):
    return lax.dot_general(
        a,
        b,
        (((contract[0],), (contract[1],)), ((), ())),
        precision=highest,
        preferred_element_type=jnp.float32,
    )


def my_place():
    scan = lax.axis_index("scan")
    tile = lax.axis_index("tile")
    return {
        "core": lax.rem(scan, 2),
        "z": lax.rem(scan // 2, 8),
        "x": lax.rem(scan // 16, 4),
        "y": (scan // 64) * 2 + tile,
    }


def device_at(place_of):
    high, low = place_of["y"] // 2, lax.rem(place_of["y"], 2)
    return (((high * 4 + place_of["x"]) * 8 + place_of["z"]) * 2 + place_of["core"], low)


def moved(here, axis, step):
    return {**here, axis: lax.rem(here[axis] + step, GRID[axis])}


def reduce_kernel(
    sums_ref,
    probe_ref,
    frame_ref,
    spec_ref,
    upd_ref,
    mix_ref,
    new_ref,
    held,
    work,
    first_a,
    first_b,
    second_a,
    second_b,
    part,
    third,
    both,
    block,
    grams,
    rows_in,
    frame,
    cols_in,
    send_sem,
    recv_sem,
):
    here = my_place()
    x, y, z, core = here["x"], here["y"], here["z"], here["core"]
    partner = moved(here, "core", 1)
    other = partner["core"]
    scan, tile = lax.axis_index("scan"), lax.axis_index("tile")
    up, down, across_tile = neighbours()
    peers = [moved(here, axis, step) for axis in ("x", "y", "z") for step in range(1, GRID[axis])]
    signal_all([device_at(peer) for peer in peers + [partner]] + [up, down])
    copies = Copies(send_sem, recv_sem)

    def send(src, dst, peer):
        return copies.send(src, dst, device_at(peer))

    def around(axis):
        return [(step, moved(here, axis, step)) for step in range(1, GRID[axis])]

    halves = []
    for low, high in SPLITS:
        rows = pl.ds(low, high - low)
        halves.append(send(sums_ref.at[other, rows], held.at[rows], partner))
    span = pl.ds(pl.multiple_of((1 - tile) * DET, DET), 3 * DET)
    from_below = copies.send(frame_ref.at[:, pl.ds(0, DET), span], rows_in.at[0], up)
    from_above = copies.send(frame_ref.at[:, pl.ds(2 * DET, DET), span], rows_in.at[1], down)
    firsts = []
    for half, (low, high) in enumerate(SPLITS):
        halves[half].wait_recv()
        rows = pl.ds(low, high - low)
        work[rows] = sums_ref[core, rows] + held[rows]
        if half == 0:
            firsts.append(
                [send(work.at[rows, p["x"]], first_a.at[i - 1], p) for i, p in around("x")]
            )
        else:
            firsts.append(
                [send(work.at[rows, :, p["y"]], first_b.at[i - 1], p) for i, p in around("y")]
            )
    seconds = []
    rows_a, rows_b = (pl.ds(low, high - low) for low, high in SPLITS)
    for copy in firsts[0]:
        copy.wait_recv()
    work[rows_a, x] += first_a[0] + first_a[1] + first_a[2]
    seconds.append([send(work.at[rows_a, x, p["y"]], second_a.at[i - 1], p) for i, p in around("y")])
    for copy in firsts[1]:
        copy.wait_recv()
    work[rows_b, :, y] += first_b[0] + first_b[1] + first_b[2]
    seconds.append([send(work.at[rows_b, p["x"], y], second_b.at[i - 1], p) for i, p in around("x")])
    for copy in seconds[0]:
        copy.wait_recv()
    part[rows_a] = work[rows_a, x, y] + second_a[0] + second_a[1] + second_a[2]
    for copy in seconds[1]:
        copy.wait_recv()
    part[rows_b] = work[rows_b, x, y] + second_b[0] + second_b[1] + second_b[2]
    part[pl.ds(13, 3)] = jnp.zeros((3, 8, DET), jnp.float32)

    thirds = [
        send(part.at[pl.ds(2 * p["z"], 2)], third.at[i - 1], p) for i, p in around("z")
    ]
    from_below.wait_recv()
    from_above.wait_recv()
    last_row = lax.axis_size("scan") - 1
    for c in range(3):
        added = jnp.where(scan == last_row, 0.0, rows_in[0, c])
        added = added + jnp.where(scan == 0, 0.0, rows_in[1, c])
        frame[c] = frame_ref[c, pl.ds(DET, DET), span] + added
    beyond = pl.ds(pl.multiple_of((1 - tile) * 2 * DET, DET), DET)
    sides = copies.send(frame.at[:, :, beyond], cols_in, across_tile)
    mine = part[pl.ds(2 * z, 2)]
    for i, copy in enumerate(thirds):
        copy.wait_recv()
        mine = mine + third[i]
    pair = pl.ds(2 * z, 2)
    both[core, pair] = mine
    backs = [send(both.at[core, pair], both.at[core, pair], p) for i, p in around("z")]
    for copy in backs:
        copy.wait_recv()
    across = send(both.at[core], both.at[core], partner)
    across.wait_recv()

    light = both[0, 12]
    power = jnp.zeros((8, DET), jnp.float32)
    for channel in range(24):
        old = probe_ref[channel, x, y]
        power = power + old * old
        new = old + both[channel // 12, channel % 12] / (light + PROBE_REG)
        block[channel // 12, pl.ds(8 * (channel % 12), 8)] = new
    for i in range(12):
        upd_ref[core, i, x, y] = block[core, pl.ds(8 * i, 8)]
    rows = jnp.concatenate(
        [
            jnp.concatenate([block[c, pl.ds(s, 12, stride=8)] for s in range(8)], axis=1)
            for c in range(2)
        ],
        axis=0,
    )
    padded = jnp.concatenate([rows, jnp.zeros((DET - 24, 8 * DET), jnp.float32)], axis=0)
    line = lax.broadcasted_iota(jnp.int32, (8, DET), 0)
    total = jnp.sum(both[1, 12], axis=0, keepdims=True)
    model = jnp.sum(power * light, axis=0, keepdims=True)
    extra = jnp.where(line == 0, total, jnp.where(line == 1, model, 0.0))
    grams[0, y] = jnp.concatenate([dot32(rows, padded, (1, 1)), extra], axis=0)

    one_a, one_b = pl.ds(0, 6), pl.ds(6, 6)
    gram_y = [send(grams.at[0, y], grams.at[0, y], p) for i, p in around("y")]
    spot_a, spot_b = upd_ref.at[core, one_a, x, y], upd_ref.at[core, one_b, x, y]
    near_a = [send(spot_a, spot_a, p) for i, p in around("y")]
    near_b = [send(spot_b, spot_b, p) for i, p in around("x")]
    for copy in gram_y:
        copy.wait_recv()
    grams[1, x] = (grams[0, 0] + grams[0, 1]) + (grams[0, 2] + grams[0, 3])
    gram_x = [send(grams.at[1, x], grams.at[1, x], p) for i, p in around("x")]
    for copy in near_a:
        copy.wait_recv()
    line_a = upd_ref.at[core, one_a, x]
    far_a = [send(line_a, line_a, p) for i, p in around("x")]
    for copy in near_b:
        copy.wait_recv()
    line_b = upd_ref.at[core, one_b, :, y]
    far_b = [send(line_b, line_b, p) for i, p in around("y")]
    last = [send(line_a, line_a, partner), send(line_b, line_b, partner)]
    for copy in gram_x:
        copy.wait_recv()
    mix_ref[...] = expanded(mixing((grams[1, 0] + grams[1, 1]) + (grams[1, 2] + grams[1, 3])))
    sides.wait_recv()
    inside = [frame[c, :, pl.ds(pl.multiple_of(tile * DET, DET), 2 * DET)] for c in range(3)]
    for c in range(3):
        left = jnp.where(tile == 1, cols_in[c], 0.0)
        right = jnp.where(tile == 0, cols_in[c], 0.0)
        inside[c] = inside[c] + jnp.concatenate([left, right], axis=1)
    for c in range(2):
        new_ref[c] = spec_ref[c] + inside[c] / (inside[2] + OBJECT_REG)
    for step in range(1, 4):
        far_a[step - 1].wait_recv()
        got = upd_ref.at[core, one_a, lax.rem(x + 4 - step, 4)]
        last.append(send(got, got, partner))
        far_b[step - 1].wait_recv()
        got = upd_ref.at[core, one_b, :, lax.rem(y + 4 - step, 4)]
        last.append(send(got, got, partner))
    for copy in last:
        copy.wait_recv()
    copies.finish()


COPIES = 58


def reduced(sums, probe, frame, specimen):
    f32 = jnp.float32
    return pl.pallas_call(
        reduce_kernel,
        out_shape=(
            jax.ShapeDtypeStruct((2, 12, 4, 4, 8, DET), f32),
            jax.ShapeDtypeStruct((192, 192), f32),
            jax.ShapeDtypeStruct(specimen.shape, f32),
        ),
        in_specs=[VMEM] * 4,
        out_specs=(VMEM,) * 3,
        scratch_shapes=[
            pltpu.VMEM((13, 4, 4, 8, DET), f32),
            pltpu.VMEM((13, 4, 4, 8, DET), f32),
            pltpu.VMEM((3, 6, 4, 8, DET), f32),
            pltpu.VMEM((3, 7, 4, 8, DET), f32),
            pltpu.VMEM((3, 6, 8, DET), f32),
            pltpu.VMEM((3, 7, 8, DET), f32),
            pltpu.VMEM((16, 8, DET), f32),
            pltpu.VMEM((7, 2, 8, DET), f32),
            pltpu.VMEM((2, 16, 8, DET), f32),
            pltpu.VMEM((2, 96, DET), f32),
            pltpu.VMEM((2, 4, 32, DET), f32),
            pltpu.VMEM((2, 3, DET, 3 * DET), f32),
            pltpu.VMEM((3, DET, 3 * DET), f32),
            pltpu.VMEM((3, DET, DET), f32),
            pltpu.SemaphoreType.DMA((COPIES,)),
            pltpu.SemaphoreType.DMA((COPIES,)),
        ],
        compiler_params=pltpu.CompilerParams(collective_id=0, has_side_effects=True, vmem_limit_bytes=LIMIT),
        name="reduce_all",
    )(sums.reshape(2, 13, 4, 4, 8, DET), probe.reshape(24, 4, 4, 8, DET), frame, specimen)


def mixing(gram):
    size = 24
    row = lax.broadcasted_iota(jnp.int32, (size, size), 0)
    col = lax.broadcasted_iota(jnp.int32, (size, size), 1)
    identity = jnp.where(row == col, 1.0, 0.0)
    even = lax.rem(row, 2) == 0
    turn = jnp.where(even & (col == row + 1), -1.0, jnp.where(~even & (col == row - 1), 1.0, 0.0))
    products = gram[:size, :size]
    embedded = products + dot32(dot32(turn, products), turn, (1, 1))
    frobenius = jnp.sqrt(jnp.sum(embedded * embedded, keepdims=True))
    current = embedded / frobenius
    inverse = identity
    for repeat in range(NS_STEPS):
        factor = 1.5 * identity - 0.5 * dot32(inverse, current)
        current = dot32(current, factor)
        inverse = dot32(factor, inverse)
    total = jnp.sum(gram[size : size + 1], keepdims=True)
    model = jnp.sum(gram[size + 1 : size + 2], keepdims=True)
    ratio = total / (model + TOTAL_EPS)
    diagonal = jnp.sum(embedded * identity, axis=1, keepdims=True)
    return inverse / jnp.sqrt(frobenius) * jnp.sqrt(ratio * diagonal)


def expanded(mix):
    tall = lax.broadcasted_iota(jnp.int32, (192, 24), 0)
    wide = lax.broadcasted_iota(jnp.int32, (192, 24), 1)
    expand = jnp.where(tall // 8 == wide, 1.0, 0.0)
    large = dot32(dot32(expand, mix), expand, (1, 1))
    row = lax.broadcasted_iota(jnp.int32, (192, 192), 0)
    col = lax.broadcasted_iota(jnp.int32, (192, 192), 1)
    return jnp.where(lax.rem(row, 8) == lax.rem(col, 8), large, 0.0)


def ortho_kernel(mix_ref, upd_ref, out_ref):
    large = mix_ref[...]
    for b in range(0, 16, 2):
        blocks = [upd_ref[:, b + i].reshape(192, DET) for i in range(2)]
        result = dot32(large, jnp.concatenate(blocks, axis=1))
        for i in range(2):
            out_ref[:, b + i] = result[:, i * DET : i * DET + DET].reshape(24, 8, DET)


def orthonormal(mix, updated):
    return pl.pallas_call(
        ortho_kernel,
        out_shape=jax.ShapeDtypeStruct((24, 16, 8, DET), jnp.float32),
        in_specs=[VMEM, VMEM],
        out_specs=VMEM,
        compiler_params=pltpu.CompilerParams(vmem_limit_bytes=LIMIT),
        name="orthonormal",
    )(mix, updated.reshape(24, 16, 8, DET))


def body(probe_modes, patterns, specimen, offsets):
    extended = extended_of(specimen)
    sums, frame = positions(offsets, probe_modes, patterns, extended)
    updated, mix, new_specimen = reduced(sums, probe_modes, frame, specimen)
    new_probe = orthonormal(mix, updated).reshape(probe_modes.shape)
    return (new_probe, new_specimen)


def solution(mesh):
    return jax.shard_map(
        body,
        mesh=mesh,
        in_specs=(
            P(),
            P(("scan", "tile"), None, None),
            P(None, "scan", "tile"),
            P(("scan", "tile"), None),
        ),
        out_specs=(P(), P(None, "scan", "tile")),
        check_vma=False,
    )
```

```python
import math

import jax
import jax.numpy as jnp
import ml_dtypes
import numpy as np
from jax import lax
from jax.experimental import pallas as pl
from jax.experimental.pallas import tpu as pltpu
from jax.sharding import PartitionSpec as P

NS_STEPS = 8
DET = 128
TALL = 136
LIMIT = 20 * 2**20
LIGHT_FLOOR = 0.05
OBJECT_REG = 0.5
PROBE_REG = 1.0
TOTAL_EPS = 1e-06
VMEM = pl.BlockSpec(memory_space=pltpu.VMEM)
SMEM = pl.BlockSpec(memory_space=pltpu.SMEM)
highest = lax.Precision.HIGHEST


def split_tables():
    index = np.arange(DET)
    angles = -2.0 * math.pi / DET * (index[:, None] * index[None, :] % DET)
    cos, sin = np.cos(angles) / math.sqrt(DET), np.sin(angles) / math.sqrt(DET)
    right = np.block([[cos, sin], [-sin, cos]])
    tables = []
    for matrix in (right, right.T):
        high = matrix.astype(ml_dtypes.bfloat16)
        low = (matrix - high.astype(np.float64)).astype(ml_dtypes.bfloat16)
        tables += [high, low]
    return jnp.asarray(np.stack(tables))


def split(value):
    high = value.astype(jnp.bfloat16)
    return high, (value - high.astype(jnp.float32)).astype(jnp.bfloat16)


def mm(a, b):
    return jnp.dot(a, b, preferred_element_type=jnp.float32)


def window_of(local_ref, position):
    row = local_ref[0, position] - (lax.axis_index("scan") - 1) * DET
    col = local_ref[1, position] - (2 * lax.axis_index("tile") - 1) * DET
    return row, col


def swapped(value):
    return jnp.concatenate(
        [
            jnp.concatenate([value[:DET, :DET], value[DET:, :DET]], axis=1),
            jnp.concatenate([value[:DET, DET:], value[DET:, DET:]], axis=1),
        ],
        axis=0,
    )


def forward_kernel(
    local_ref,
    probe_ref,
    patterns_ref,
    ext_ref,
    tables_ref,
    high_ref,
    low_ref,
    patch_ref,
    extra_ref,
    light_ref,
    far_ref,
):
    modes = probe_ref.shape[0]
    pairs = modes // 2
    rh_ref, rl_ref, lh_ref, ll_ref = (tables_ref.at[i] for i in range(4))
    power = jnp.zeros((DET, DET), jnp.float32)
    for k in range(modes):
        power = power + probe_ref[k, 0] * probe_ref[k, 0] + probe_ref[k, 1] * probe_ref[k, 1]
    extra_ref[...] = jnp.zeros_like(extra_ref)
    light_ref[...] = jnp.zeros_like(light_ref)
    for position in range(patterns_ref.shape[0]):
        row, col = window_of(local_ref, position)
        column = jnp.minimum(col // DET, 2)
        slab = jnp.minimum(row // 8, 31)
        shift, drop = col - column * DET, row - slab * 8
        rows, cols = pl.ds(pl.multiple_of(slab * 8, 8), TALL), pl.ds(pl.multiple_of(column * DET, DET), 2 * DET)
        for c in range(2):
            window = pltpu.roll(ext_ref[c, rows, cols], lax.rem(2 * DET - shift, 2 * DET), 1)[:, :DET]
            patch_ref[position, c] = pltpu.roll(window, lax.rem(TALL - drop, TALL), 0)[:DET]
        value = jnp.concatenate([power, jnp.zeros((8, DET), jnp.float32)], axis=0)
        value = pltpu.roll(value, drop, 0)
        value = jnp.concatenate([value, jnp.zeros_like(value)], axis=1)
        light_ref[rows, cols] += pltpu.roll(value, shift, 1)
        ar, ai = patch_ref[position, 0], patch_ref[position, 1]
        extra_ref[0] += ar * ar + ai * ai
        extra_ref[1] += patterns_ref[position]

    def one_position(position, _):
        model = jnp.zeros((DET, DET), jnp.float32)
        for j in range(pairs):
            lefts = []
            for k in (2 * j, 2 * j + 1):
                pr, pi = probe_ref[k, 0], probe_ref[k, 1]
                ar, ai = patch_ref[position, 0], patch_ref[position, 1]
                lefts.append(jnp.concatenate([pr * ar - pi * ai, pr * ai + pi * ar], axis=1))
            xh, xl = split(jnp.concatenate(lefts, axis=0))
            half = mm(xh, rh_ref[...]) + mm(xl, rh_ref[...]) + mm(xh, rl_ref[...])
            yh, yl = split(swapped(half))
            far = mm(lh_ref[...], yh) + mm(lh_ref[...], yl) + mm(ll_ref[...], yh)
            far_ref[j] = far
            squares = far * far
            squares = squares[:DET] + squares[DET:]
            model = model + squares[:, :DET] + squares[:, DET:]
        factor = jnp.sqrt(patterns_ref[position]) / jnp.sqrt(jnp.maximum(model, LIGHT_FLOOR)) - 1.0
        wide = jnp.concatenate([factor, factor], axis=1)
        wide = jnp.concatenate([wide, wide], axis=0)
        for j in range(pairs):
            high_ref[position, j], low_ref[position, j] = split(far_ref[j] * wide)
        return 0

    lax.fori_loop(0, patterns_ref.shape[0], one_position, 0)


def forward(local, probe, patterns, extended, tables):
    count, pairs = patterns.shape[0], probe.shape[0] // 2
    spectra = jax.ShapeDtypeStruct((count, pairs, 2 * DET, 2 * DET), jnp.bfloat16)
    return pl.pallas_call(
        forward_kernel,
        out_shape=(
            spectra,
            spectra,
            jax.ShapeDtypeStruct((count, 2, DET, DET), jnp.float32),
            jax.ShapeDtypeStruct((2, DET, DET), jnp.float32),
            jax.ShapeDtypeStruct(extended.shape[1:], jnp.float32),
        ),
        in_specs=[SMEM] + [VMEM] * 4,
        out_specs=(VMEM,) * 5,
        scratch_shapes=[pltpu.VMEM((pairs, 2 * DET, 2 * DET), jnp.float32)],
        compiler_params=pltpu.CompilerParams(vmem_limit_bytes=LIMIT),
        name="forward",
    )(local, probe, patterns, extended, tables)


def signal_all(peers):
    barrier = pltpu.get_barrier_semaphore()
    for peer in peers:
        pl.semaphore_signal(barrier, inc=1, device_id=peer, device_id_type=pl.DeviceIdType.MESH)
    return lambda: pl.semaphore_wait(barrier, len(peers))


class Copies:
    def __init__(self, send_sem, recv_sem):
        self.send_sem, self.recv_sem, self.started = send_sem, recv_sem, []

    def send(self, src, dst, device):
        index = len(self.started)
        copy = pltpu.make_async_remote_copy(
            src_ref=src,
            dst_ref=dst,
            send_sem=self.send_sem.at[index],
            recv_sem=self.recv_sem.at[index],
            device_id=device,
            device_id_type=pl.DeviceIdType.MESH,
        )
        copy.start()
        self.started.append(copy)
        return copy

    def finish(self):
        for copy in self.started:
            copy.wait_send()


def neighbours():
    scan, tile = lax.axis_index("scan"), lax.axis_index("tile")
    size = lax.axis_size("scan")
    up = (lax.rem(scan + size - 1, size), tile)
    down = (lax.rem(scan + 1, size), tile)
    return up, down, (scan, 1 - tile)


def halo_kernel(spec_ref, constants_ref, ext_ref, tables_ref, send_sem, recv_sem):
    scan, tile = lax.axis_index("scan"), lax.axis_index("tile")
    up, down, across = neighbours()
    ready = signal_all([up, down, across])
    copies = Copies(send_sem, recv_sem)
    own, above, below = pl.ds(DET, DET), pl.ds(0, DET), pl.ds(2 * DET, DET)
    middle = pl.ds(DET, 2 * DET)
    given = pl.ds(pl.multiple_of((1 - tile) * DET, DET), DET)
    empty = pl.ds(pl.multiple_of(tile * 3 * DET, DET), DET)
    filled = pl.ds(pl.multiple_of((1 - tile) * 3 * DET, DET), DET)
    ready()
    pieces = [(c, r * 64) for c in range(2) for r in range(2)]
    side = [
        copies.send(
            spec_ref.at[c, pl.ds(r, 64), given], ext_ref.at[c, pl.ds(DET + r, 64), empty], across
        )
        for c, r in pieces
    ]
    rest = [
        copies.send(spec_ref, ext_ref.at[:, below, middle], up),
        copies.send(spec_ref, ext_ref.at[:, above, middle], down),
    ]
    ext_ref[:, own, middle] = spec_ref[...]
    tables_ref[...] = constants_ref[...]
    ext_ref[:, :, empty] = jnp.zeros((2, 3 * DET, DET), jnp.float32)
    for (c, r), copy in zip(pieces, side):
        copy.wait_recv()
        corner = ext_ref.at[c, pl.ds(DET + r, 64), filled]
        rest.append(copies.send(corner, ext_ref.at[c, pl.ds(2 * DET + r, 64), filled], up))
        rest.append(copies.send(corner, ext_ref.at[c, pl.ds(r, 64), filled], down))
    for copy in rest:
        copy.wait_recv()

    @pl.when(scan == 0)
    def _():
        ext_ref[:, above] = jnp.zeros((2, DET, 4 * DET), jnp.float32)

    @pl.when(scan == lax.axis_size("scan") - 1)
    def _():
        ext_ref[:, below] = jnp.zeros((2, DET, 4 * DET), jnp.float32)

    copies.finish()


def extended_of(specimen):
    return pl.pallas_call(
        halo_kernel,
        out_shape=(
            jax.ShapeDtypeStruct((2, 3 * DET, 4 * DET), jnp.float32),
            jax.ShapeDtypeStruct((4, 2 * DET, 2 * DET), jnp.bfloat16),
        ),
        in_specs=[VMEM, VMEM],
        out_specs=(VMEM, VMEM),
        scratch_shapes=[
            pltpu.SemaphoreType.DMA((14,)),
            pltpu.SemaphoreType.DMA((14,)),
        ],
        compiler_params=pltpu.CompilerParams(collective_id=1, has_side_effects=True, vmem_limit_bytes=LIMIT),
        name="halo",
    )(specimen, split_tables())


SPLITS = ((0, 6), (6, 13))
AXES = ("x", "y")
GRID = {"x": 4, "y": 4, "z": 8, "core": 2}


def dot32(a, b, contract=(1, 0)):
    return lax.dot_general(
        a,
        b,
        (((contract[0],), (contract[1],)), ((), ())),
        precision=highest,
        preferred_element_type=jnp.float32,
    )


def my_place():
    scan = lax.axis_index("scan")
    tile = lax.axis_index("tile")
    return {
        "core": lax.rem(scan, 2),
        "z": lax.rem(scan // 2, 8),
        "x": lax.rem(scan // 16, 4),
        "y": (scan // 64) * 2 + tile,
    }


def device_at(place_of):
    high, low = place_of["y"] // 2, lax.rem(place_of["y"], 2)
    return (((high * 4 + place_of["x"]) * 8 + place_of["z"]) * 2 + place_of["core"], low)


def moved(here, axis, step):
    return {**here, axis: lax.rem(here[axis] + step, GRID[axis])}


def slot_channel(slot):
    mode = 2 * (slot // 2) if slot < 6 else 2 * ((slot - 6) // 2) + 1
    return 2 * mode + slot % 2


def reduce_kernel(
    local_ref,
    high_ref,
    low_ref,
    patch_ref,
    extra_ref,
    light_ref,
    tables_ref,
    probe_ref,
    upd_ref,
    mix_ref,
    inside_ref,
    given,
    held,
    work,
    num_ref,
    canvas,
    first_a,
    first_b,
    second_a,
    second_b,
    part,
    third,
    both,
    block,
    grams,
    rows_in,
    frame,
    cols_in,
    send_sem,
    recv_sem,
):
    here = my_place()
    x, y, z, core = here["x"], here["y"], here["z"], here["core"]
    partner = moved(here, "core", 1)
    other = partner["core"]
    scan, tile = lax.axis_index("scan"), lax.axis_index("tile")
    up, down, across_tile = neighbours()
    peers = [moved(here, axis, step) for axis in ("x", "y", "z") for step in range(1, GRID[axis])]
    ready = signal_all([device_at(peer) for peer in peers + [partner]] + [up, down])
    copies = Copies(send_sem, recv_sem)

    def send(src, dst, peer):
        return copies.send(src, dst, device_at(peer))

    def around(axis):
        return [(step, moved(here, axis, step)) for step in range(1, GRID[axis])]

    rh_ref, rl_ref, lh_ref, ll_ref = (tables_ref.at[i] for i in range(4))
    count = patch_ref.shape[0]
    num_ref[...] = jnp.zeros_like(num_ref)

    def pair_step(side, pair, target):
        slots = [2 * pair, 2 * pair + 1, 6 + 2 * pair, 7 + 2 * pair]
        for slot in slots:
            target[slot] = jnp.zeros((4, 4, 8, DET), jnp.float32)

        def two_positions(step, _):
            totals = [None] * 4
            for q in range(2):
                p = 2 * step + q
                bh, bl = high_ref[p, 3 * side + pair], low_ref[p, 3 * side + pair]
                back = mm(rh_ref[...], bh) + mm(rh_ref[...], bl) + mm(rl_ref[...], bh)
                zh, zl = split(swapped(back))
                change = mm(zh, lh_ref[...]) + mm(zl, lh_ref[...]) + mm(zh, ll_ref[...])
                ar, ai = patch_ref[p, 0], patch_ref[p, 1]
                for i in range(2):
                    channel = 12 * side + 4 * pair + 2 * i
                    cr = change[i * DET : i * DET + DET, :DET]
                    ci = change[i * DET : i * DET + DET, DET:]
                    pr = probe_ref[channel].reshape(DET, DET)
                    pi = probe_ref[channel + 1].reshape(DET, DET)
                    for c, value in enumerate((ar * cr + ai * ci, ar * ci - ai * cr)):
                        old = totals[2 * i + c]
                        totals[2 * i + c] = value if old is None else old + value
                    num_ref[p, 0] += pr * cr + pi * ci
                    num_ref[p, 1] += pr * ci - pi * cr
            for slot, total in zip(slots, totals):
                target[slot] += total.reshape(4, 4, 8, DET)
            return 0

        lax.fori_loop(0, count // 2, two_positions, 0)

    def slots_of(pair):
        return pl.ds(2 * pair, 2), pl.ds(6 + 2 * pair, 2)

    span = pl.ds(pl.multiple_of((1 - tile) * DET, DET), 3 * DET)
    top, bottom = pl.ds(0, DET), pl.ds(2 * DET, DET)
    halves, firsts_a, firsts_b = [], [], []
    last_slot = pl.ds(12, 1)

    for pair in range(3):
        pair_step(other, pair, given)
        if pair == 0:
            ready()
            extra_half = send(extra_ref.at[pl.ds(other, 1)], held.at[last_slot], partner)
            lights = [
                copies.send(light_ref.at[top, span], rows_in.at[0, 2], up),
                copies.send(light_ref.at[bottom, span], rows_in.at[1, 2], down),
            ]
        halves.append([send(given.at[s], held.at[s], partner) for s in slots_of(pair)])
    extra_half.wait_recv()
    work[12] = extra_ref[core] + held[12]
    firsts_e = [send(work.at[last_slot, :, p["y"]], first_b.at[i - 1, pl.ds(6, 1)], p) for i, p in around("y")]

    def fold_first(low, size, low_b, size_b):
        rows, rows_b = pl.ds(low, size), pl.ds(6 + low_b, size_b)
        from_b = pl.ds(low_b, size_b)
        work[rows, x] += first_a[0, rows] + first_a[1, rows] + first_a[2, rows]
        work[rows_b, :, y] += first_b[0, from_b] + first_b[1, from_b] + first_b[2, from_b]
        a = [send(work.at[rows, x, p["y"]], second_a.at[i - 1, rows], p) for i, p in around("y")]
        b = [send(work.at[rows_b, p["x"], y], second_b.at[i - 1, from_b], p) for i, p in around("x")]
        return a + b

    for pair in range(3):
        pair_step(core, pair, work)
        rows_a, rows_b = slots_of(pair)
        for copy, rows in zip(halves[pair], (rows_a, rows_b)):
            copy.wait_recv()
            work[rows] += held[rows]
        firsts_a.append(
            [send(work.at[rows_a, p["x"]], first_a.at[i - 1, rows_a], p) for i, p in around("x")]
        )
        firsts_b.append(
            [send(work.at[rows_b, :, p["y"]], first_b.at[i - 1, rows_a], p) for i, p in around("y")]
        )
    for copy in firsts_a[0] + firsts_a[1] + firsts_b[0] + firsts_b[1]:
        copy.wait_recv()
    seconds = fold_first(0, 4, 0, 4)

    wide, tall = [], []
    for p in range(count):
        row, col = window_of(local_ref, p)
        values = jnp.concatenate([num_ref[p, 0], num_ref[p, 1]], axis=0)
        high, low = split(values)
        place = lax.broadcasted_iota(jnp.int32, (DET, 4 * DET), 0) + col
        across_shift = place == lax.broadcasted_iota(jnp.int32, (DET, 4 * DET), 1)
        across_shift = jnp.where(across_shift, 1.0, 0.0).astype(jnp.bfloat16)
        wide.append(split(mm(high, across_shift) + mm(low, across_shift)))
        place = lax.broadcasted_iota(jnp.int32, (3 * DET, DET), 1) + row
        down_shift = place == lax.broadcasted_iota(jnp.int32, (3 * DET, DET), 0)
        tall.append(jnp.where(down_shift, 1.0, 0.0).astype(jnp.bfloat16))
    down_shift = jnp.concatenate(tall, axis=1)
    for c in range(2):
        high = jnp.concatenate([w[0][c * DET : c * DET + DET] for w in wide], axis=0)
        low = jnp.concatenate([w[1][c * DET : c * DET + DET] for w in wide], axis=0)
        canvas[c] = mm(down_shift, high) + mm(down_shift, low)
    rows_out = [
        copies.send(canvas.at[:, top, span], rows_in.at[0, pl.ds(0, 2)], up),
        copies.send(canvas.at[:, bottom, span], rows_in.at[1, pl.ds(0, 2)], down),
    ]

    for copy in firsts_a[2] + firsts_b[2] + firsts_e:
        copy.wait_recv()
    seconds += fold_first(4, 2, 4, 3)
    for copy in seconds:
        copy.wait_recv()
    rows_a, rows_b = (pl.ds(low, high - low) for low, high in SPLITS)
    part[rows_a] = work[rows_a, x, y] + second_a[0] + second_a[1] + second_a[2]
    part[rows_b] = work[rows_b, x, y] + second_b[0] + second_b[1] + second_b[2]
    part[pl.ds(13, 3)] = jnp.zeros((3, 8, DET), jnp.float32)

    thirds = [
        send(part.at[pl.ds(2 * p["z"], 2)], third.at[i - 1], p) for i, p in around("z")
    ]
    for copy in lights + rows_out:
        copy.wait_recv()
    last_row = lax.axis_size("scan") - 1
    for c in range(3):
        added = jnp.where(scan == last_row, 0.0, rows_in[0, c])
        added = added + jnp.where(scan == 0, 0.0, rows_in[1, c])
        own = canvas[c, pl.ds(DET, DET), span] if c < 2 else light_ref[pl.ds(DET, DET), span]
        frame[c] = own + added
    beyond = pl.ds(pl.multiple_of((1 - tile) * 2 * DET, DET), DET)
    sides = copies.send(frame.at[:, :, beyond], cols_in, across_tile)
    mine = part[pl.ds(2 * z, 2)]
    for i, copy in enumerate(thirds):
        copy.wait_recv()
        mine = mine + third[i]
    pair = pl.ds(2 * z, 2)
    both[core, pair] = mine
    backs = [send(both.at[core, pair], both.at[core, pair], p) for i, p in around("z")]
    for copy in backs:
        copy.wait_recv()
    across = send(both.at[core], both.at[core], partner)
    across.wait_recv()

    light = both[0, 12]
    power = jnp.zeros((8, DET), jnp.float32)
    for c in range(2):
        for slot in range(12):
            old = probe_ref[12 * c + slot_channel(slot), x, y]
            power = power + old * old
            block[c, pl.ds(8 * slot, 8)] = old + both[c, slot] / (light + PROBE_REG)
    for i in range(12):
        upd_ref[core, i, x, y] = block[core, pl.ds(8 * i, 8)]
    rows = jnp.concatenate(
        [
            jnp.concatenate([block[c, pl.ds(s, 12, stride=8)] for s in range(8)], axis=1)
            for c in range(2)
        ],
        axis=0,
    )
    padded = jnp.concatenate([rows, jnp.zeros((DET - 24, 8 * DET), jnp.float32)], axis=0)
    line = lax.broadcasted_iota(jnp.int32, (8, DET), 0)
    total = jnp.sum(both[1, 12], axis=0, keepdims=True)
    model = jnp.sum(power * light, axis=0, keepdims=True)
    extra = jnp.where(line == 0, total, jnp.where(line == 1, model, 0.0))
    grams[0, y] = jnp.concatenate([dot32(rows, padded, (1, 1)), extra], axis=0)

    one_a, one_b = pl.ds(0, 6), pl.ds(6, 6)
    gram_y = [send(grams.at[0, y], grams.at[0, y], p) for i, p in around("y")]
    spot_a, spot_b = upd_ref.at[core, one_a, x, y], upd_ref.at[core, one_b, x, y]
    near_a = [send(spot_a, spot_a, p) for i, p in around("y")]
    near_b = [send(spot_b, spot_b, p) for i, p in around("x")]
    for copy in gram_y:
        copy.wait_recv()
    grams[1, x] = (grams[0, 0] + grams[0, 1]) + (grams[0, 2] + grams[0, 3])
    gram_x = [send(grams.at[1, x], grams.at[1, x], p) for i, p in around("x")]
    for copy in near_a:
        copy.wait_recv()
    line_a = upd_ref.at[core, one_a, x]
    far_a = [send(line_a, line_a, p) for i, p in around("x")]
    for copy in near_b:
        copy.wait_recv()
    line_b = upd_ref.at[core, one_b, :, y]
    far_b = [send(line_b, line_b, p) for i, p in around("y")]
    last = [send(line_a, line_a, partner), send(line_b, line_b, partner)]
    for copy in gram_x:
        copy.wait_recv()
    mix_ref[...] = expanded(mixing((grams[1, 0] + grams[1, 1]) + (grams[1, 2] + grams[1, 3])))
    sides.wait_recv()
    for c in range(3):
        left = jnp.where(tile == 1, cols_in[c], 0.0)
        right = jnp.where(tile == 0, cols_in[c], 0.0)
        own = frame[c, :, pl.ds(pl.multiple_of(tile * DET, DET), 2 * DET)]
        inside_ref[c] = own + jnp.concatenate([left, right], axis=1)
    for step in range(1, 4):
        far_a[step - 1].wait_recv()
        got = upd_ref.at[core, one_a, lax.rem(x + 4 - step, 4)]
        last.append(send(got, got, partner))
        far_b[step - 1].wait_recv()
        got = upd_ref.at[core, one_b, :, lax.rem(y + 4 - step, 4)]
        last.append(send(got, got, partner))
    for copy in last:
        copy.wait_recv()
    copies.finish()


COPIES = 96


def reduced(local, spectra, tables, probe):
    f32 = jnp.float32
    high, low, patches, extra, light = spectra
    return pl.pallas_call(
        reduce_kernel,
        out_shape=(
            jax.ShapeDtypeStruct((2, 12, 4, 4, 8, DET), f32),
            jax.ShapeDtypeStruct((192, 192), f32),
            jax.ShapeDtypeStruct((3, DET, 2 * DET), f32),
        ),
        in_specs=[SMEM] + [VMEM] * 7,
        out_specs=(VMEM,) * 3,
        scratch_shapes=[
            pltpu.VMEM((12, 4, 4, 8, DET), f32),
            pltpu.VMEM((13, 4, 4, 8, DET), f32),
            pltpu.VMEM((13, 4, 4, 8, DET), f32),
            pltpu.VMEM((4, 2, DET, DET), f32),
            pltpu.VMEM((2, 3 * DET, 4 * DET), f32),
            pltpu.VMEM((3, 6, 4, 8, DET), f32),
            pltpu.VMEM((3, 7, 4, 8, DET), f32),
            pltpu.VMEM((3, 6, 8, DET), f32),
            pltpu.VMEM((3, 7, 8, DET), f32),
            pltpu.VMEM((16, 8, DET), f32),
            pltpu.VMEM((7, 2, 8, DET), f32),
            pltpu.VMEM((2, 16, 8, DET), f32),
            pltpu.VMEM((2, 96, DET), f32),
            pltpu.VMEM((2, 4, 32, DET), f32),
            pltpu.VMEM((2, 3, DET, 3 * DET), f32),
            pltpu.VMEM((3, DET, 3 * DET), f32),
            pltpu.VMEM((3, DET, DET), f32),
            pltpu.SemaphoreType.DMA((COPIES,)),
            pltpu.SemaphoreType.DMA((COPIES,)),
        ],
        compiler_params=pltpu.CompilerParams(
            collective_id=0, has_side_effects=True, vmem_limit_bytes=LIMIT
        ),
        name="reduce_all",
    )(
        local,
        high,
        low,
        patches,
        extra.reshape(2, 4, 4, 8, DET),
        light,
        tables,
        probe.reshape(24, 4, 4, 8, DET),
    )


def mixing(gram):
    size = 24
    row = lax.broadcasted_iota(jnp.int32, (size, size), 0)
    col = lax.broadcasted_iota(jnp.int32, (size, size), 1)
    identity = jnp.where(row == col, 1.0, 0.0)
    even = lax.rem(row, 2) == 0
    turn = jnp.where(even & (col == row + 1), -1.0, jnp.where(~even & (col == row - 1), 1.0, 0.0))
    products = gram[:size, :size]
    embedded = products + dot32(dot32(turn, products), turn, (1, 1))
    frobenius = jnp.sqrt(jnp.sum(embedded * embedded, keepdims=True))
    current = embedded / frobenius
    inverse = identity
    for repeat in range(NS_STEPS):
        factor = 1.5 * identity - 0.5 * dot32(inverse, current)
        current = dot32(current, factor)
        inverse = dot32(factor, inverse)
    total = jnp.sum(gram[size : size + 1], keepdims=True)
    model = jnp.sum(gram[size + 1 : size + 2], keepdims=True)
    ratio = total / (model + TOTAL_EPS)
    diagonal = jnp.sum(embedded * identity, axis=1, keepdims=True)
    return inverse / jnp.sqrt(frobenius) * jnp.sqrt(ratio * diagonal)


def expanded(mix):
    tall = lax.broadcasted_iota(jnp.int32, (192, 24), 0)
    wide = lax.broadcasted_iota(jnp.int32, (192, 24), 1)
    expand = jnp.where(tall // 8 == wide, 1.0, 0.0)
    large = dot32(dot32(expand, mix), expand, (1, 1))
    row = lax.broadcasted_iota(jnp.int32, (192, 192), 0)
    col = lax.broadcasted_iota(jnp.int32, (192, 192), 1)
    return jnp.where(lax.rem(row, 8) == lax.rem(col, 8), large, 0.0)


def finish_kernel(mix_ref, upd_ref, inside_ref, spec_ref, out_ref, new_ref):
    large = mix_ref[...]
    for b in range(0, 16, 2):
        blocks = [upd_ref[:, b + i].reshape(192, DET) for i in range(2)]
        result = dot32(large, jnp.concatenate(blocks, axis=1))
        for i in range(2):
            block = result[:, i * DET : i * DET + DET].reshape(24, 8, DET)
            for c in range(2):
                for slot in range(12):
                    out_ref[12 * c + slot_channel(slot), b + i] = block[12 * c + slot]
    for c in range(2):
        new_ref[c] = spec_ref[c] + inside_ref[c] / (inside_ref[2] + OBJECT_REG)


def finished(mix, updated, inside, specimen):
    return pl.pallas_call(
        finish_kernel,
        out_shape=(
            jax.ShapeDtypeStruct((24, 16, 8, DET), jnp.float32),
            jax.ShapeDtypeStruct(specimen.shape, jnp.float32),
        ),
        in_specs=[VMEM] * 4,
        out_specs=(VMEM, VMEM),
        compiler_params=pltpu.CompilerParams(vmem_limit_bytes=LIMIT),
        name="finish",
    )(mix, updated.reshape(24, 16, 8, DET), inside, specimen)


def body(probe_modes, patterns, specimen, offsets):
    local = offsets.T
    extended, tables = extended_of(specimen)
    spectra = forward(local, probe_modes, patterns, extended, tables)
    updated, mix, inside = reduced(local, spectra, tables, probe_modes)
    new_probe, new_specimen = finished(mix, updated, inside, specimen)
    return (new_probe.reshape(probe_modes.shape), new_specimen)


def solution(mesh):
    return jax.shard_map(
        body,
        mesh=mesh,
        in_specs=(
            P(),
            P(("scan", "tile"), None, None),
            P(None, "scan", "tile"),
            P(("scan", "tile"), None),
        ),
        out_specs=(P(), P(None, "scan", "tile")),
        check_vma=False,
    )
```

```python
import math

import jax
import jax.numpy as jnp
import ml_dtypes
import numpy as np
from jax import lax
from jax.experimental import pallas as pl
from jax.experimental.pallas import tpu as pltpu
from jax.sharding import PartitionSpec as P

NS_STEPS = 8
DET = 128
TALL = 136
LIMIT = 20 * 2**20
FLOPS_PER_US = 10**9
BYTES_PER_US = 3 * 10**6
LIGHT_FLOOR = 0.05
OBJECT_REG = 0.5
PROBE_REG = 1.0
TOTAL_EPS = 1e-06
VMEM = pl.BlockSpec(memory_space=pltpu.VMEM)
SMEM = pl.BlockSpec(memory_space=pltpu.SMEM)
highest = lax.Precision.HIGHEST


def cost(microseconds):
    return pl.CostEstimate(
        flops=int(microseconds * FLOPS_PER_US),
        bytes_accessed=int(microseconds * BYTES_PER_US),
        transcendentals=0,
    )


def split_tables():
    index = np.arange(DET)
    angles = -2.0 * math.pi / DET * (index[:, None] * index[None, :] % DET)
    cos, sin = np.cos(angles) / math.sqrt(DET), np.sin(angles) / math.sqrt(DET)
    right = np.block([[cos, sin], [-sin, cos]])
    tables = []
    for matrix in (right, right.T):
        high = matrix.astype(ml_dtypes.bfloat16)
        low = (matrix - high.astype(np.float64)).astype(ml_dtypes.bfloat16)
        tables += [high, low]
    return jnp.asarray(np.stack(tables))


def split(value):
    high = value.astype(jnp.bfloat16)
    return high, (value - high.astype(jnp.float32)).astype(jnp.bfloat16)


def mm(a, b):
    return jnp.dot(a, b, preferred_element_type=jnp.float32)


def window_of(local_ref, position):
    row = local_ref[0, position] - (lax.axis_index("scan") - 1) * DET
    col = local_ref[1, position] - (2 * lax.axis_index("tile") - 1) * DET
    return row, col


def swapped(value):
    return jnp.concatenate(
        [
            jnp.concatenate([value[:DET, :DET], value[DET:, :DET]], axis=1),
            jnp.concatenate([value[:DET, DET:], value[DET:, DET:]], axis=1),
        ],
        axis=0,
    )


def forward_kernel(
    local_ref,
    probe_ref,
    patterns_ref,
    ext_ref,
    tables_ref,
    high_ref,
    low_ref,
    patch_ref,
    extra_ref,
    light_ref,
    far_ref,
):
    modes = probe_ref.shape[0]
    pairs = modes // 2
    rh_ref, rl_ref, lh_ref, ll_ref = (tables_ref.at[i] for i in range(4))
    power = jnp.zeros((DET, DET), jnp.float32)
    for k in range(modes):
        power = power + probe_ref[k, 0] * probe_ref[k, 0] + probe_ref[k, 1] * probe_ref[k, 1]
    extra_ref[...] = jnp.zeros_like(extra_ref)
    light_ref[...] = jnp.zeros_like(light_ref)
    for position in range(patterns_ref.shape[0]):
        row, col = window_of(local_ref, position)
        column = jnp.minimum(col // DET, 2)
        slab = jnp.minimum(row // 8, 31)
        shift, drop = col - column * DET, row - slab * 8
        rows, cols = pl.ds(pl.multiple_of(slab * 8, 8), TALL), pl.ds(pl.multiple_of(column * DET, DET), 2 * DET)
        for c in range(2):
            window = pltpu.roll(ext_ref[c, rows, cols], lax.rem(2 * DET - shift, 2 * DET), 1)[:, :DET]
            patch_ref[position, c] = pltpu.roll(window, lax.rem(TALL - drop, TALL), 0)[:DET]
        value = jnp.concatenate([power, jnp.zeros((8, DET), jnp.float32)], axis=0)
        value = pltpu.roll(value, drop, 0)
        value = jnp.concatenate([value, jnp.zeros_like(value)], axis=1)
        light_ref[rows, cols] += pltpu.roll(value, shift, 1)
        ar, ai = patch_ref[position, 0], patch_ref[position, 1]
        extra_ref[0] += ar * ar + ai * ai
        extra_ref[1] += patterns_ref[position]

    def one_position(position, _):
        model = jnp.zeros((DET, DET), jnp.float32)
        for j in range(pairs):
            lefts = []
            for k in (2 * j, 2 * j + 1):
                pr, pi = probe_ref[k, 0], probe_ref[k, 1]
                ar, ai = patch_ref[position, 0], patch_ref[position, 1]
                lefts.append(jnp.concatenate([pr * ar - pi * ai, pr * ai + pi * ar], axis=1))
            xh, xl = split(jnp.concatenate(lefts, axis=0))
            half = mm(xh, rh_ref[...]) + mm(xl, rh_ref[...]) + mm(xh, rl_ref[...])
            yh, yl = split(swapped(half))
            far = mm(lh_ref[...], yh) + mm(lh_ref[...], yl) + mm(ll_ref[...], yh)
            far_ref[j] = far
            squares = far * far
            squares = squares[:DET] + squares[DET:]
            model = model + squares[:, :DET] + squares[:, DET:]
        factor = jnp.sqrt(patterns_ref[position]) / jnp.sqrt(jnp.maximum(model, LIGHT_FLOOR)) - 1.0
        wide = jnp.concatenate([factor, factor], axis=1)
        wide = jnp.concatenate([wide, wide], axis=0)
        for j in range(pairs):
            high_ref[position, j], low_ref[position, j] = split(far_ref[j] * wide)
        return 0

    lax.fori_loop(0, patterns_ref.shape[0], one_position, 0)


def forward(local, probe, patterns, extended, tables):
    count, pairs = patterns.shape[0], probe.shape[0] // 2
    spectra = jax.ShapeDtypeStruct((count, pairs, 2 * DET, 2 * DET), jnp.bfloat16)
    return pl.pallas_call(
        forward_kernel,
        out_shape=(
            spectra,
            spectra,
            jax.ShapeDtypeStruct((count, 2, DET, DET), jnp.float32),
            jax.ShapeDtypeStruct((2, DET, DET), jnp.float32),
            jax.ShapeDtypeStruct(extended.shape[1:], jnp.float32),
        ),
        in_specs=[SMEM] + [VMEM] * 4,
        out_specs=(VMEM,) * 5,
        cost_estimate=cost(9),
        scratch_shapes=[pltpu.VMEM((pairs, 2 * DET, 2 * DET), jnp.float32)],
        compiler_params=pltpu.CompilerParams(vmem_limit_bytes=LIMIT),
        name="forward",
    )(local, probe, patterns, extended, tables)


def signal_all(peers):
    barrier = pltpu.get_barrier_semaphore()
    for peer in peers:
        pl.semaphore_signal(barrier, inc=1, device_id=peer, device_id_type=pl.DeviceIdType.MESH)
    return lambda: pl.semaphore_wait(barrier, len(peers))


class Copies:
    def __init__(self, send_sem, recv_sem):
        self.send_sem, self.recv_sem, self.started = send_sem, recv_sem, []

    def send(self, src, dst, device):
        index = len(self.started)
        copy = pltpu.make_async_remote_copy(
            src_ref=src,
            dst_ref=dst,
            send_sem=self.send_sem.at[index],
            recv_sem=self.recv_sem.at[index],
            device_id=device,
            device_id_type=pl.DeviceIdType.MESH,
        )
        copy.start()
        self.started.append(copy)
        return copy

    def finish(self):
        for copy in self.started:
            copy.wait_send()


def neighbours():
    scan, tile = lax.axis_index("scan"), lax.axis_index("tile")
    size = lax.axis_size("scan")
    up = (lax.rem(scan + size - 1, size), tile)
    down = (lax.rem(scan + 1, size), tile)
    return up, down, (scan, 1 - tile)


def halo_kernel(spec_ref, ext_ref, send_sem, recv_sem):
    scan, tile = lax.axis_index("scan"), lax.axis_index("tile")
    up, down, across = neighbours()
    ready = signal_all([up, down, across])
    copies = Copies(send_sem, recv_sem)
    own, above, below = pl.ds(DET, DET), pl.ds(0, DET), pl.ds(2 * DET, DET)
    middle = pl.ds(DET, 2 * DET)
    given = pl.ds(pl.multiple_of((1 - tile) * DET, DET), DET)
    empty = pl.ds(pl.multiple_of(tile * 3 * DET, DET), DET)
    filled = pl.ds(pl.multiple_of((1 - tile) * 3 * DET, DET), DET)
    ready()
    pieces = [(c, r * 64) for c in range(2) for r in range(2)]
    side = [
        copies.send(
            spec_ref.at[c, pl.ds(r, 64), given], ext_ref.at[c, pl.ds(DET + r, 64), empty], across
        )
        for c, r in pieces
    ]
    rest = [
        copies.send(spec_ref, ext_ref.at[:, below, middle], up),
        copies.send(spec_ref, ext_ref.at[:, above, middle], down),
    ]
    ext_ref[:, own, middle] = spec_ref[...]
    ext_ref[:, :, empty] = jnp.zeros((2, 3 * DET, DET), jnp.float32)
    for (c, r), copy in zip(pieces, side):
        copy.wait_recv()
        corner = ext_ref.at[c, pl.ds(DET + r, 64), filled]
        rest.append(copies.send(corner, ext_ref.at[c, pl.ds(2 * DET + r, 64), filled], up))
        rest.append(copies.send(corner, ext_ref.at[c, pl.ds(r, 64), filled], down))
    for copy in rest:
        copy.wait_recv()

    @pl.when(scan == 0)
    def _():
        ext_ref[:, above] = jnp.zeros((2, DET, 4 * DET), jnp.float32)

    @pl.when(scan == lax.axis_size("scan") - 1)
    def _():
        ext_ref[:, below] = jnp.zeros((2, DET, 4 * DET), jnp.float32)

    copies.finish()


def extended_of(specimen):
    return pl.pallas_call(
        halo_kernel,
        out_shape=jax.ShapeDtypeStruct((2, 3 * DET, 4 * DET), jnp.float32),
        in_specs=[VMEM],
        out_specs=VMEM,
        cost_estimate=cost(8),
        scratch_shapes=[
            pltpu.SemaphoreType.DMA((14,)),
            pltpu.SemaphoreType.DMA((14,)),
        ],
        compiler_params=pltpu.CompilerParams(collective_id=1, has_side_effects=True, vmem_limit_bytes=LIMIT),
        name="halo",
    )(specimen)


SPLITS = ((0, 6), (6, 13))
AXES = ("x", "y")
GRID = {"x": 4, "y": 4, "z": 8, "core": 2}


def dot32(a, b, contract=(1, 0)):
    return lax.dot_general(
        a,
        b,
        (((contract[0],), (contract[1],)), ((), ())),
        precision=highest,
        preferred_element_type=jnp.float32,
    )


def my_place():
    scan = lax.axis_index("scan")
    tile = lax.axis_index("tile")
    return {
        "core": lax.rem(scan, 2),
        "z": lax.rem(scan // 2, 8),
        "x": lax.rem(scan // 16, 4),
        "y": (scan // 64) * 2 + tile,
    }


def device_at(place_of):
    high, low = place_of["y"] // 2, lax.rem(place_of["y"], 2)
    return (((high * 4 + place_of["x"]) * 8 + place_of["z"]) * 2 + place_of["core"], low)


def moved(here, axis, step):
    return {**here, axis: lax.rem(here[axis] + step, GRID[axis])}


def slot_channel(slot):
    mode = 2 * (slot // 2) if slot < 6 else 2 * ((slot - 6) // 2) + 1
    return 2 * mode + slot % 2


def reduce_kernel(
    local_ref,
    high_ref,
    low_ref,
    patch_ref,
    extra_ref,
    light_ref,
    tables_ref,
    probe_ref,
    upd_ref,
    mix_ref,
    inside_ref,
    given,
    held,
    work,
    num_ref,
    canvas,
    first_a,
    first_b,
    second_a,
    second_b,
    part,
    third,
    both,
    block,
    grams,
    rows_in,
    frame,
    cols_in,
    send_sem,
    recv_sem,
):
    here = my_place()
    x, y, z, core = here["x"], here["y"], here["z"], here["core"]
    partner = moved(here, "core", 1)
    other = partner["core"]
    scan, tile = lax.axis_index("scan"), lax.axis_index("tile")
    up, down, across_tile = neighbours()
    peers = [moved(here, axis, step) for axis in ("x", "y", "z") for step in range(1, GRID[axis])]
    ready = signal_all([device_at(peer) for peer in peers + [partner]] + [up, down])
    copies = Copies(send_sem, recv_sem)

    def send(src, dst, peer):
        return copies.send(src, dst, device_at(peer))

    def around(axis):
        return [(step, moved(here, axis, step)) for step in range(1, GRID[axis])]

    rh_ref, rl_ref, lh_ref, ll_ref = (tables_ref.at[i] for i in range(4))
    count = patch_ref.shape[0]
    num_ref[...] = jnp.zeros_like(num_ref)

    def pair_step(side, pair, target):
        slots = [2 * pair, 2 * pair + 1, 6 + 2 * pair, 7 + 2 * pair]
        for slot in slots:
            target[slot] = jnp.zeros((4, 4, 8, DET), jnp.float32)

        def two_positions(step, _):
            totals = [None] * 4
            for q in range(2):
                p = 2 * step + q
                bh, bl = high_ref[p, 3 * side + pair], low_ref[p, 3 * side + pair]
                back = mm(rh_ref[...], bh) + mm(rh_ref[...], bl) + mm(rl_ref[...], bh)
                zh, zl = split(swapped(back))
                change = mm(zh, lh_ref[...]) + mm(zl, lh_ref[...]) + mm(zh, ll_ref[...])
                ar, ai = patch_ref[p, 0], patch_ref[p, 1]
                for i in range(2):
                    channel = 12 * side + 4 * pair + 2 * i
                    cr = change[i * DET : i * DET + DET, :DET]
                    ci = change[i * DET : i * DET + DET, DET:]
                    pr = probe_ref[channel].reshape(DET, DET)
                    pi = probe_ref[channel + 1].reshape(DET, DET)
                    for c, value in enumerate((ar * cr + ai * ci, ar * ci - ai * cr)):
                        old = totals[2 * i + c]
                        totals[2 * i + c] = value if old is None else old + value
                    num_ref[p, 0] += pr * cr + pi * ci
                    num_ref[p, 1] += pr * ci - pi * cr
            for slot, total in zip(slots, totals):
                target[slot] += total.reshape(4, 4, 8, DET)
            return 0

        lax.fori_loop(0, count // 2, two_positions, 0)

    def slots_of(pair):
        return pl.ds(2 * pair, 2), pl.ds(6 + 2 * pair, 2)

    span = pl.ds(pl.multiple_of((1 - tile) * DET, DET), 3 * DET)
    top, bottom = pl.ds(0, DET), pl.ds(2 * DET, DET)
    halves, firsts_a, firsts_b = [], [], []
    last_slot = pl.ds(12, 1)

    for pair in range(3):
        pair_step(other, pair, given)
        if pair == 0:
            ready()
            extra_half = send(extra_ref.at[pl.ds(other, 1)], held.at[last_slot], partner)
            lights = [
                copies.send(light_ref.at[top, span], rows_in.at[0, 2], up),
                copies.send(light_ref.at[bottom, span], rows_in.at[1, 2], down),
            ]
        halves.append([send(given.at[s], held.at[s], partner) for s in slots_of(pair)])
    extra_half.wait_recv()
    work[12] = extra_ref[core] + held[12]
    firsts_e = [send(work.at[last_slot, :, p["y"]], first_b.at[i - 1, pl.ds(6, 1)], p) for i, p in around("y")]

    def fold_first(low, size, low_b, size_b):
        rows, rows_b = pl.ds(low, size), pl.ds(6 + low_b, size_b)
        from_b = pl.ds(low_b, size_b)
        work[rows, x] += first_a[0, rows] + first_a[1, rows] + first_a[2, rows]
        work[rows_b, :, y] += first_b[0, from_b] + first_b[1, from_b] + first_b[2, from_b]
        a = [send(work.at[rows, x, p["y"]], second_a.at[i - 1, rows], p) for i, p in around("y")]
        b = [send(work.at[rows_b, p["x"], y], second_b.at[i - 1, from_b], p) for i, p in around("x")]
        return a + b

    for pair in range(3):
        pair_step(core, pair, work)
        rows_a, rows_b = slots_of(pair)
        for copy, rows in zip(halves[pair], (rows_a, rows_b)):
            copy.wait_recv()
            work[rows] += held[rows]
        firsts_a.append(
            [send(work.at[rows_a, p["x"]], first_a.at[i - 1, rows_a], p) for i, p in around("x")]
        )
        firsts_b.append(
            [send(work.at[rows_b, :, p["y"]], first_b.at[i - 1, rows_a], p) for i, p in around("y")]
        )
    for copy in firsts_a[0] + firsts_a[1] + firsts_b[0] + firsts_b[1]:
        copy.wait_recv()
    seconds = fold_first(0, 4, 0, 4)

    wide, tall = [], []
    for p in range(count):
        row, col = window_of(local_ref, p)
        values = jnp.concatenate([num_ref[p, 0], num_ref[p, 1]], axis=0)
        high, low = split(values)
        place = lax.broadcasted_iota(jnp.int32, (DET, 4 * DET), 0) + col
        across_shift = place == lax.broadcasted_iota(jnp.int32, (DET, 4 * DET), 1)
        across_shift = jnp.where(across_shift, 1.0, 0.0).astype(jnp.bfloat16)
        wide.append(split(mm(high, across_shift) + mm(low, across_shift)))
        place = lax.broadcasted_iota(jnp.int32, (3 * DET, DET), 1) + row
        down_shift = place == lax.broadcasted_iota(jnp.int32, (3 * DET, DET), 0)
        tall.append(jnp.where(down_shift, 1.0, 0.0).astype(jnp.bfloat16))
    down_shift = jnp.concatenate(tall, axis=1)
    for c in range(2):
        high = jnp.concatenate([w[0][c * DET : c * DET + DET] for w in wide], axis=0)
        low = jnp.concatenate([w[1][c * DET : c * DET + DET] for w in wide], axis=0)
        canvas[c] = mm(down_shift, high) + mm(down_shift, low)
    rows_out = [
        copies.send(canvas.at[:, top, span], rows_in.at[0, pl.ds(0, 2)], up),
        copies.send(canvas.at[:, bottom, span], rows_in.at[1, pl.ds(0, 2)], down),
    ]

    for copy in firsts_a[2] + firsts_b[2] + firsts_e:
        copy.wait_recv()
    seconds += fold_first(4, 2, 4, 3)
    for copy in seconds:
        copy.wait_recv()
    rows_a, rows_b = (pl.ds(low, high - low) for low, high in SPLITS)
    part[rows_a] = work[rows_a, x, y] + second_a[0] + second_a[1] + second_a[2]
    part[rows_b] = work[rows_b, x, y] + second_b[0] + second_b[1] + second_b[2]
    part[pl.ds(13, 3)] = jnp.zeros((3, 8, DET), jnp.float32)

    thirds = [
        send(part.at[pl.ds(2 * p["z"], 2)], third.at[i - 1], p) for i, p in around("z")
    ]
    for copy in lights + rows_out:
        copy.wait_recv()
    last_row = lax.axis_size("scan") - 1
    for c in range(3):
        added = jnp.where(scan == last_row, 0.0, rows_in[0, c])
        added = added + jnp.where(scan == 0, 0.0, rows_in[1, c])
        own = canvas[c, pl.ds(DET, DET), span] if c < 2 else light_ref[pl.ds(DET, DET), span]
        frame[c] = own + added
    beyond = pl.ds(pl.multiple_of((1 - tile) * 2 * DET, DET), DET)
    sides = copies.send(frame.at[:, :, beyond], cols_in, across_tile)
    mine = part[pl.ds(2 * z, 2)]
    for i, copy in enumerate(thirds):
        copy.wait_recv()
        mine = mine + third[i]
    pair = pl.ds(2 * z, 2)
    both[core, pair] = mine
    backs = [send(both.at[core, pair], both.at[core, pair], p) for i, p in around("z")]
    for copy in backs:
        copy.wait_recv()
    across = send(both.at[core], both.at[core], partner)
    across.wait_recv()

    light = both[0, 12]
    power = jnp.zeros((8, DET), jnp.float32)
    for c in range(2):
        for slot in range(12):
            old = probe_ref[12 * c + slot_channel(slot), x, y]
            power = power + old * old
            block[c, pl.ds(8 * slot, 8)] = old + both[c, slot] / (light + PROBE_REG)
    for i in range(12):
        upd_ref[core, i, x, y] = block[core, pl.ds(8 * i, 8)]
    rows = jnp.concatenate(
        [
            jnp.concatenate([block[c, pl.ds(s, 12, stride=8)] for s in range(8)], axis=1)
            for c in range(2)
        ],
        axis=0,
    )
    padded = jnp.concatenate([rows, jnp.zeros((DET - 24, 8 * DET), jnp.float32)], axis=0)
    line = lax.broadcasted_iota(jnp.int32, (8, DET), 0)
    total = jnp.sum(both[1, 12], axis=0, keepdims=True)
    model = jnp.sum(power * light, axis=0, keepdims=True)
    extra = jnp.where(line == 0, total, jnp.where(line == 1, model, 0.0))
    grams[0, y] = jnp.concatenate([dot32(rows, padded, (1, 1)), extra], axis=0)

    one_a, one_b = pl.ds(0, 6), pl.ds(6, 6)
    gram_y = [send(grams.at[0, y], grams.at[0, y], p) for i, p in around("y")]
    spot_a, spot_b = upd_ref.at[core, one_a, x, y], upd_ref.at[core, one_b, x, y]
    near_a = [send(spot_a, spot_a, p) for i, p in around("y")]
    near_b = [send(spot_b, spot_b, p) for i, p in around("x")]
    for copy in gram_y:
        copy.wait_recv()
    grams[1, x] = (grams[0, 0] + grams[0, 1]) + (grams[0, 2] + grams[0, 3])
    gram_x = [send(grams.at[1, x], grams.at[1, x], p) for i, p in around("x")]
    for copy in near_a:
        copy.wait_recv()
    line_a = upd_ref.at[core, one_a, x]
    far_a = [send(line_a, line_a, p) for i, p in around("x")]
    for copy in near_b:
        copy.wait_recv()
    line_b = upd_ref.at[core, one_b, :, y]
    far_b = [send(line_b, line_b, p) for i, p in around("y")]
    last = [send(line_a, line_a, partner), send(line_b, line_b, partner)]
    for copy in gram_x:
        copy.wait_recv()
    mix_ref[...] = expanded(mixing((grams[1, 0] + grams[1, 1]) + (grams[1, 2] + grams[1, 3])))
    sides.wait_recv()
    for c in range(3):
        left = jnp.where(tile == 1, cols_in[c], 0.0)
        right = jnp.where(tile == 0, cols_in[c], 0.0)
        own = frame[c, :, pl.ds(pl.multiple_of(tile * DET, DET), 2 * DET)]
        inside_ref[c] = own + jnp.concatenate([left, right], axis=1)
    for step in range(1, 4):
        far_a[step - 1].wait_recv()
        got = upd_ref.at[core, one_a, lax.rem(x + 4 - step, 4)]
        last.append(send(got, got, partner))
        far_b[step - 1].wait_recv()
        got = upd_ref.at[core, one_b, :, lax.rem(y + 4 - step, 4)]
        last.append(send(got, got, partner))
    for copy in last:
        copy.wait_recv()
    copies.finish()


COPIES = 96


def reduced(local, spectra, tables, probe):
    f32 = jnp.float32
    high, low, patches, extra, light = spectra
    return pl.pallas_call(
        reduce_kernel,
        out_shape=(
            jax.ShapeDtypeStruct((2, 12, 4, 4, 8, DET), f32),
            jax.ShapeDtypeStruct((192, 192), f32),
            jax.ShapeDtypeStruct((3, DET, 2 * DET), f32),
        ),
        in_specs=[SMEM] + [VMEM] * 7,
        cost_estimate=cost(45),
        out_specs=(VMEM,) * 3,
        scratch_shapes=[
            pltpu.VMEM((12, 4, 4, 8, DET), f32),
            pltpu.VMEM((13, 4, 4, 8, DET), f32),
            pltpu.VMEM((13, 4, 4, 8, DET), f32),
            pltpu.VMEM((4, 2, DET, DET), f32),
            pltpu.VMEM((2, 3 * DET, 4 * DET), f32),
            pltpu.VMEM((3, 6, 4, 8, DET), f32),
            pltpu.VMEM((3, 7, 4, 8, DET), f32),
            pltpu.VMEM((3, 6, 8, DET), f32),
            pltpu.VMEM((3, 7, 8, DET), f32),
            pltpu.VMEM((16, 8, DET), f32),
            pltpu.VMEM((7, 2, 8, DET), f32),
            pltpu.VMEM((2, 16, 8, DET), f32),
            pltpu.VMEM((2, 96, DET), f32),
            pltpu.VMEM((2, 4, 32, DET), f32),
            pltpu.VMEM((2, 3, DET, 3 * DET), f32),
            pltpu.VMEM((3, DET, 3 * DET), f32),
            pltpu.VMEM((3, DET, DET), f32),
            pltpu.SemaphoreType.DMA((COPIES,)),
            pltpu.SemaphoreType.DMA((COPIES,)),
        ],
        compiler_params=pltpu.CompilerParams(
            collective_id=0, has_side_effects=True, vmem_limit_bytes=LIMIT
        ),
        name="reduce_all",
    )(
        local,
        high,
        low,
        patches,
        extra.reshape(2, 4, 4, 8, DET),
        light,
        tables,
        probe.reshape(24, 4, 4, 8, DET),
    )


def mixing(gram):
    size = 24
    row = lax.broadcasted_iota(jnp.int32, (size, size), 0)
    col = lax.broadcasted_iota(jnp.int32, (size, size), 1)
    identity = jnp.where(row == col, 1.0, 0.0)
    even = lax.rem(row, 2) == 0
    turn = jnp.where(even & (col == row + 1), -1.0, jnp.where(~even & (col == row - 1), 1.0, 0.0))
    products = gram[:size, :size]
    embedded = products + dot32(dot32(turn, products), turn, (1, 1))
    frobenius = jnp.sqrt(jnp.sum(embedded * embedded, keepdims=True))
    current = embedded / frobenius
    inverse = identity
    for repeat in range(NS_STEPS):
        factor = 1.5 * identity - 0.5 * dot32(inverse, current)
        current = dot32(current, factor)
        inverse = dot32(factor, inverse)
    total = jnp.sum(gram[size : size + 1], keepdims=True)
    model = jnp.sum(gram[size + 1 : size + 2], keepdims=True)
    ratio = total / (model + TOTAL_EPS)
    diagonal = jnp.sum(embedded * identity, axis=1, keepdims=True)
    return inverse / jnp.sqrt(frobenius) * jnp.sqrt(ratio * diagonal)


def expanded(mix):
    tall = lax.broadcasted_iota(jnp.int32, (192, 24), 0)
    wide = lax.broadcasted_iota(jnp.int32, (192, 24), 1)
    expand = jnp.where(tall // 8 == wide, 1.0, 0.0)
    large = dot32(dot32(expand, mix), expand, (1, 1))
    row = lax.broadcasted_iota(jnp.int32, (192, 192), 0)
    col = lax.broadcasted_iota(jnp.int32, (192, 192), 1)
    return jnp.where(lax.rem(row, 8) == lax.rem(col, 8), large, 0.0)


def finish_kernel(mix_ref, upd_ref, inside_ref, spec_ref, out_ref, new_ref):
    large = mix_ref[...]
    for b in range(0, 16, 2):
        blocks = [upd_ref[:, b + i].reshape(192, DET) for i in range(2)]
        result = dot32(large, jnp.concatenate(blocks, axis=1))
        for i in range(2):
            block = result[:, i * DET : i * DET + DET].reshape(24, 8, DET)
            for c in range(2):
                for slot in range(12):
                    out_ref[12 * c + slot_channel(slot), b + i] = block[12 * c + slot]
    for c in range(2):
        new_ref[c] = spec_ref[c] + inside_ref[c] / (inside_ref[2] + OBJECT_REG)


def finished(mix, updated, inside, specimen):
    return pl.pallas_call(
        finish_kernel,
        out_shape=(
            jax.ShapeDtypeStruct((24, 16, 8, DET), jnp.float32),
            jax.ShapeDtypeStruct(specimen.shape, jnp.float32),
        ),
        in_specs=[VMEM] * 4,
        out_specs=(VMEM, VMEM),
        cost_estimate=cost(3),
        compiler_params=pltpu.CompilerParams(vmem_limit_bytes=LIMIT),
        name="finish",
    )(mix, updated.reshape(24, 16, 8, DET), inside, specimen)


def body(probe_modes, patterns, specimen, offsets):
    local = offsets.T
    extended, tables = extended_of(specimen), split_tables()
    spectra = forward(local, probe_modes, patterns, extended, tables)
    updated, mix, inside = reduced(local, spectra, tables, probe_modes)
    new_probe, new_specimen = finished(mix, updated, inside, specimen)
    return (new_probe.reshape(probe_modes.shape), new_specimen)


def solution(mesh):
    return jax.shard_map(
        body,
        mesh=mesh,
        in_specs=(
            P(),
            P(("scan", "tile"), None, None),
            P(None, "scan", "tile"),
            P(("scan", "tile"), None),
        ),
        out_specs=(P(), P(None, "scan", "tile")),
        check_vma=False,
    )
```

```python
import math

import jax
import jax.numpy as jnp
import ml_dtypes
import numpy as np
from jax import lax
from jax.experimental import pallas as pl
from jax.experimental.pallas import tpu as pltpu
from jax.sharding import PartitionSpec as P

NS_STEPS = 8
DET = 128
TALL = 136
LIMIT = 20 * 2**20
FLOPS_PER_US = 10**9
BYTES_PER_US = 3 * 10**6
LIGHT_FLOOR = 0.05
OBJECT_REG = 0.5
PROBE_REG = 1.0
TOTAL_EPS = 1e-06
VMEM = pl.BlockSpec(memory_space=pltpu.VMEM)
SMEM = pl.BlockSpec(memory_space=pltpu.SMEM)
highest = lax.Precision.HIGHEST


def cost(microseconds):
    return pl.CostEstimate(
        flops=int(microseconds * FLOPS_PER_US),
        bytes_accessed=int(microseconds * BYTES_PER_US),
        transcendentals=0,
    )


def split_tables():
    index = np.arange(DET)
    angles = -2.0 * math.pi / DET * (index[:, None] * index[None, :] % DET)
    cos, sin = np.cos(angles) / math.sqrt(DET), np.sin(angles) / math.sqrt(DET)
    right = np.block([[cos, sin], [-sin, cos]])
    tables = []
    for matrix in (right, right.T):
        high = matrix.astype(ml_dtypes.bfloat16)
        low = (matrix - high.astype(np.float64)).astype(ml_dtypes.bfloat16)
        tables += [high, low]
    return jnp.asarray(np.stack(tables))


def split(value):
    high = value.astype(jnp.bfloat16)
    return high, (value - high.astype(jnp.float32)).astype(jnp.bfloat16)


def mm(a, b):
    return jnp.dot(a, b, preferred_element_type=jnp.float32)


def window_of(local_ref, position):
    row = local_ref[0, position] - (lax.axis_index("scan") - 1) * DET
    col = local_ref[1, position] - (2 * lax.axis_index("tile") - 1) * DET
    return row, col


def swapped(value):
    return jnp.concatenate(
        [
            jnp.concatenate([value[:DET, :DET], value[DET:, :DET]], axis=1),
            jnp.concatenate([value[:DET, DET:], value[DET:, DET:]], axis=1),
        ],
        axis=0,
    )


def forward_kernel(
    local_ref,
    probe_ref,
    patterns_ref,
    ext_ref,
    tables_ref,
    high_ref,
    low_ref,
    patch_ref,
    extra_ref,
    light_ref,
    far_ref,
    half_high,
    half_low,
):
    modes = probe_ref.shape[0]
    pairs = modes // 2
    rh_ref, rl_ref, lh_ref, ll_ref = (tables_ref.at[i] for i in range(4))
    power = jnp.zeros((DET, DET), jnp.float32)
    for k in range(modes):
        power = power + probe_ref[k, 0] * probe_ref[k, 0] + probe_ref[k, 1] * probe_ref[k, 1]
    extra_ref[...] = jnp.zeros_like(extra_ref)
    light_ref[...] = jnp.zeros_like(light_ref)
    for position in range(patterns_ref.shape[0]):
        row, col = window_of(local_ref, position)
        column = jnp.minimum(col // DET, 2)
        slab = jnp.minimum(row // 8, 31)
        shift, drop = col - column * DET, row - slab * 8
        rows, cols = pl.ds(pl.multiple_of(slab * 8, 8), TALL), pl.ds(pl.multiple_of(column * DET, DET), 2 * DET)
        for c in range(2):
            window = pltpu.roll(ext_ref[c, rows, cols], lax.rem(2 * DET - shift, 2 * DET), 1)[:, :DET]
            patch_ref[position, c] = pltpu.roll(window, lax.rem(TALL - drop, TALL), 0)[:DET]
        value = jnp.concatenate([power, jnp.zeros((8, DET), jnp.float32)], axis=0)
        value = pltpu.roll(value, drop, 0)
        value = jnp.concatenate([value, jnp.zeros_like(value)], axis=1)
        light_ref[rows, cols] += pltpu.roll(value, shift, 1)
        ar, ai = patch_ref[position, 0], patch_ref[position, 1]
        extra_ref[0] += ar * ar + ai * ai
        extra_ref[1] += patterns_ref[position]

    def one_position(position, _):
        ar, ai = patch_ref[position, 0], patch_ref[position, 1]
        for j in range(pairs):
            lefts = []
            for k in (2 * j, 2 * j + 1):
                pr, pi = probe_ref[k, 0], probe_ref[k, 1]
                lefts.append(jnp.concatenate([pr * ar - pi * ai, pr * ai + pi * ar], axis=1))
            xh, xl = split(jnp.concatenate(lefts, axis=0))
            half = mm(xh, rh_ref[...]) + mm(xl, rh_ref[...]) + mm(xh, rl_ref[...])
            half_high[j], half_low[j] = split(swapped(half))
        model = jnp.zeros((DET, DET), jnp.float32)
        for j in range(pairs):
            yh, yl = half_high[j], half_low[j]
            far = mm(lh_ref[...], yh) + mm(lh_ref[...], yl) + mm(ll_ref[...], yh)
            far_ref[j] = far
            squares = far * far
            squares = squares[:DET] + squares[DET:]
            model = model + squares[:, :DET] + squares[:, DET:]
        factor = jnp.sqrt(patterns_ref[position]) / jnp.sqrt(jnp.maximum(model, LIGHT_FLOOR)) - 1.0
        wide = jnp.concatenate([factor, factor], axis=1)
        wide = jnp.concatenate([wide, wide], axis=0)
        for j in range(pairs):
            high_ref[position, j], low_ref[position, j] = split(far_ref[j] * wide)
        return 0

    lax.fori_loop(0, patterns_ref.shape[0], one_position, 0)


def forward(local, probe, patterns, extended, tables):
    count, pairs = patterns.shape[0], probe.shape[0] // 2
    spectra = jax.ShapeDtypeStruct((count, pairs, 2 * DET, 2 * DET), jnp.bfloat16)
    return pl.pallas_call(
        forward_kernel,
        out_shape=(
            spectra,
            spectra,
            jax.ShapeDtypeStruct((count, 2, DET, DET), jnp.float32),
            jax.ShapeDtypeStruct((2, DET, DET), jnp.float32),
            jax.ShapeDtypeStruct(extended.shape[1:], jnp.float32),
        ),
        in_specs=[SMEM] + [VMEM] * 4,
        out_specs=(VMEM,) * 5,
        cost_estimate=cost(9),
        scratch_shapes=[
            pltpu.VMEM((pairs, 2 * DET, 2 * DET), jnp.float32),
            pltpu.VMEM((pairs, 2 * DET, 2 * DET), jnp.bfloat16),
            pltpu.VMEM((pairs, 2 * DET, 2 * DET), jnp.bfloat16),
        ],
        compiler_params=pltpu.CompilerParams(vmem_limit_bytes=LIMIT),
        name="forward",
    )(local, probe, patterns, extended, tables)


def signal_all(peers):
    barrier = pltpu.get_barrier_semaphore()
    for peer in peers:
        pl.semaphore_signal(barrier, inc=1, device_id=peer, device_id_type=pl.DeviceIdType.MESH)
    return lambda: pl.semaphore_wait(barrier, len(peers))


class Copies:
    def __init__(self, send_sem, recv_sem):
        self.send_sem, self.recv_sem, self.started = send_sem, recv_sem, []

    def send(self, src, dst, device):
        index = len(self.started)
        copy = pltpu.make_async_remote_copy(
            src_ref=src,
            dst_ref=dst,
            send_sem=self.send_sem.at[index],
            recv_sem=self.recv_sem.at[index],
            device_id=device,
            device_id_type=pl.DeviceIdType.MESH,
        )
        copy.start()
        self.started.append(copy)
        return copy

    def finish(self):
        for copy in self.started:
            copy.wait_send()


def neighbours():
    scan, tile = lax.axis_index("scan"), lax.axis_index("tile")
    size = lax.axis_size("scan")
    up = (lax.rem(scan + size - 1, size), tile)
    down = (lax.rem(scan + 1, size), tile)
    return up, down, (scan, 1 - tile)


def halo_kernel(spec_ref, ext_ref, send_sem, recv_sem):
    scan, tile = lax.axis_index("scan"), lax.axis_index("tile")
    up, down, across = neighbours()
    ready = signal_all([up, down, across])
    copies = Copies(send_sem, recv_sem)
    own, above, below = pl.ds(DET, DET), pl.ds(0, DET), pl.ds(2 * DET, DET)
    middle = pl.ds(DET, 2 * DET)
    given = pl.ds(pl.multiple_of((1 - tile) * DET, DET), DET)
    empty = pl.ds(pl.multiple_of(tile * 3 * DET, DET), DET)
    filled = pl.ds(pl.multiple_of((1 - tile) * 3 * DET, DET), DET)
    ready()
    pieces = [(c, r * 64) for c in range(2) for r in range(2)]
    side = [
        copies.send(
            spec_ref.at[c, pl.ds(r, 64), given], ext_ref.at[c, pl.ds(DET + r, 64), empty], across
        )
        for c, r in pieces
    ]
    rest = [
        copies.send(spec_ref, ext_ref.at[:, below, middle], up),
        copies.send(spec_ref, ext_ref.at[:, above, middle], down),
    ]
    ext_ref[:, own, middle] = spec_ref[...]
    ext_ref[:, :, empty] = jnp.zeros((2, 3 * DET, DET), jnp.float32)
    for (c, r), copy in zip(pieces, side):
        copy.wait_recv()
        corner = ext_ref.at[c, pl.ds(DET + r, 64), filled]
        rest.append(copies.send(corner, ext_ref.at[c, pl.ds(2 * DET + r, 64), filled], up))
        rest.append(copies.send(corner, ext_ref.at[c, pl.ds(r, 64), filled], down))
    for copy in rest:
        copy.wait_recv()

    @pl.when(scan == 0)
    def _():
        ext_ref[:, above] = jnp.zeros((2, DET, 4 * DET), jnp.float32)

    @pl.when(scan == lax.axis_size("scan") - 1)
    def _():
        ext_ref[:, below] = jnp.zeros((2, DET, 4 * DET), jnp.float32)

    copies.finish()


def extended_of(specimen):
    return pl.pallas_call(
        halo_kernel,
        out_shape=jax.ShapeDtypeStruct((2, 3 * DET, 4 * DET), jnp.float32),
        in_specs=[VMEM],
        out_specs=VMEM,
        cost_estimate=cost(8),
        scratch_shapes=[
            pltpu.SemaphoreType.DMA((14,)),
            pltpu.SemaphoreType.DMA((14,)),
        ],
        compiler_params=pltpu.CompilerParams(collective_id=1, has_side_effects=True, vmem_limit_bytes=LIMIT),
        name="halo",
    )(specimen)


SPLITS = ((0, 6), (6, 13))
AXES = ("x", "y")
GRID = {"x": 4, "y": 4, "z": 8, "core": 2}


def dot32(a, b, contract=(1, 0)):
    return lax.dot_general(
        a,
        b,
        (((contract[0],), (contract[1],)), ((), ())),
        precision=highest,
        preferred_element_type=jnp.float32,
    )


def my_place():
    scan = lax.axis_index("scan")
    tile = lax.axis_index("tile")
    return {
        "core": lax.rem(scan, 2),
        "z": lax.rem(scan // 2, 8),
        "x": lax.rem(scan // 16, 4),
        "y": (scan // 64) * 2 + tile,
    }


def device_at(place_of):
    high, low = place_of["y"] // 2, lax.rem(place_of["y"], 2)
    return (((high * 4 + place_of["x"]) * 8 + place_of["z"]) * 2 + place_of["core"], low)


def moved(here, axis, step):
    return {**here, axis: lax.rem(here[axis] + step, GRID[axis])}


def slot_channel(slot):
    mode = 2 * (slot // 2) if slot < 6 else 2 * ((slot - 6) // 2) + 1
    return 2 * mode + slot % 2


def reduce_kernel(
    local_ref,
    high_ref,
    low_ref,
    patch_ref,
    extra_ref,
    light_ref,
    tables_ref,
    probe_ref,
    upd_ref,
    mix_ref,
    inside_ref,
    given,
    held,
    work,
    num_ref,
    back_high,
    back_low,
    canvas,
    first_a,
    first_b,
    second_a,
    second_b,
    part,
    third,
    both,
    block,
    grams,
    rows_in,
    frame,
    cols_in,
    send_sem,
    recv_sem,
):
    here = my_place()
    x, y, z, core = here["x"], here["y"], here["z"], here["core"]
    partner = moved(here, "core", 1)
    other = partner["core"]
    scan, tile = lax.axis_index("scan"), lax.axis_index("tile")
    up, down, across_tile = neighbours()
    peers = [moved(here, axis, step) for axis in ("x", "y", "z") for step in range(1, GRID[axis])]
    ready = signal_all([device_at(peer) for peer in peers + [partner]] + [up, down])
    copies = Copies(send_sem, recv_sem)

    def send(src, dst, peer):
        return copies.send(src, dst, device_at(peer))

    def around(axis):
        return [(step, moved(here, axis, step)) for step in range(1, GRID[axis])]

    rh_ref, rl_ref, lh_ref, ll_ref = (tables_ref.at[i] for i in range(4))
    count = patch_ref.shape[0]
    num_ref[...] = jnp.zeros_like(num_ref)

    def pair_step(side, pair, target):
        slots = [2 * pair, 2 * pair + 1, 6 + 2 * pair, 7 + 2 * pair]
        for p in range(count):
            bh, bl = high_ref[p, 3 * side + pair], low_ref[p, 3 * side + pair]
            back = mm(rh_ref[...], bh) + mm(rh_ref[...], bl) + mm(rl_ref[...], bh)
            back_high[p], back_low[p] = split(swapped(back))
        for p in range(count):
            zh, zl = back_high[p], back_low[p]
            change = mm(zh, lh_ref[...]) + mm(zl, lh_ref[...]) + mm(zh, ll_ref[...])
            ar, ai = patch_ref[p, 0], patch_ref[p, 1]
            nums = [num_ref[p, 0], num_ref[p, 1]]
            for i in range(2):
                channel = 12 * side + 4 * pair + 2 * i
                cr = change[i * DET : i * DET + DET, :DET]
                ci = change[i * DET : i * DET + DET, DET:]
                pr = probe_ref[channel].reshape(DET, DET)
                pi = probe_ref[channel + 1].reshape(DET, DET)
                for c, value in enumerate((ar * cr + ai * ci, ar * ci - ai * cr)):
                    value = value.reshape(4, 4, 8, DET)
                    slot = slots[2 * i + c]
                    target[slot] = value if p == 0 else target[slot] + value
                nums[0] += pr * cr + pi * ci
                nums[1] += pr * ci - pi * cr
            num_ref[p, 0], num_ref[p, 1] = nums

    def slots_of(pair):
        return pl.ds(2 * pair, 2), pl.ds(6 + 2 * pair, 2)

    span = pl.ds(pl.multiple_of((1 - tile) * DET, DET), 3 * DET)
    top, bottom = pl.ds(0, DET), pl.ds(2 * DET, DET)
    halves, firsts_a, firsts_b = [], [], []
    last_slot = pl.ds(12, 1)

    for pair in range(3):
        pair_step(other, pair, given)
        if pair == 0:
            ready()
            extra_half = send(extra_ref.at[pl.ds(other, 1)], held.at[last_slot], partner)
            lights = [
                copies.send(light_ref.at[top, span], rows_in.at[0, 2], up),
                copies.send(light_ref.at[bottom, span], rows_in.at[1, 2], down),
            ]
        halves.append([send(given.at[s], held.at[s], partner) for s in slots_of(pair)])
    extra_half.wait_recv()
    work[12] = extra_ref[core] + held[12]
    firsts_e = [send(work.at[last_slot, :, p["y"]], first_b.at[i - 1, pl.ds(6, 1)], p) for i, p in around("y")]

    def fold_first(low, size, low_b, size_b):
        rows, rows_b = pl.ds(low, size), pl.ds(6 + low_b, size_b)
        from_b = pl.ds(low_b, size_b)
        work[rows, x] += first_a[0, rows] + first_a[1, rows] + first_a[2, rows]
        work[rows_b, :, y] += first_b[0, from_b] + first_b[1, from_b] + first_b[2, from_b]
        a = [send(work.at[rows, x, p["y"]], second_a.at[i - 1, rows], p) for i, p in around("y")]
        b = [send(work.at[rows_b, p["x"], y], second_b.at[i - 1, from_b], p) for i, p in around("x")]
        return a + b

    for pair in range(3):
        pair_step(core, pair, work)
        rows_a, rows_b = slots_of(pair)
        for copy, rows in zip(halves[pair], (rows_a, rows_b)):
            copy.wait_recv()
            work[rows] += held[rows]
        firsts_a.append(
            [send(work.at[rows_a, p["x"]], first_a.at[i - 1, rows_a], p) for i, p in around("x")]
        )
        firsts_b.append(
            [send(work.at[rows_b, :, p["y"]], first_b.at[i - 1, rows_a], p) for i, p in around("y")]
        )
    for copy in firsts_a[0] + firsts_a[1] + firsts_b[0] + firsts_b[1]:
        copy.wait_recv()
    seconds = fold_first(0, 4, 0, 4)

    wide, tall = [], []
    for p in range(count):
        row, col = window_of(local_ref, p)
        values = jnp.concatenate([num_ref[p, 0], num_ref[p, 1]], axis=0)
        high, low = split(values)
        place = lax.broadcasted_iota(jnp.int32, (DET, 4 * DET), 0) + col
        across_shift = place == lax.broadcasted_iota(jnp.int32, (DET, 4 * DET), 1)
        across_shift = jnp.where(across_shift, 1.0, 0.0).astype(jnp.bfloat16)
        wide.append(split(mm(high, across_shift) + mm(low, across_shift)))
        place = lax.broadcasted_iota(jnp.int32, (3 * DET, DET), 1) + row
        down_shift = place == lax.broadcasted_iota(jnp.int32, (3 * DET, DET), 0)
        tall.append(jnp.where(down_shift, 1.0, 0.0).astype(jnp.bfloat16))
    down_shift = jnp.concatenate(tall, axis=1)
    for c in range(2):
        high = jnp.concatenate([w[0][c * DET : c * DET + DET] for w in wide], axis=0)
        low = jnp.concatenate([w[1][c * DET : c * DET + DET] for w in wide], axis=0)
        canvas[c] = mm(down_shift, high) + mm(down_shift, low)
    rows_out = [
        copies.send(canvas.at[:, top, span], rows_in.at[0, pl.ds(0, 2)], up),
        copies.send(canvas.at[:, bottom, span], rows_in.at[1, pl.ds(0, 2)], down),
    ]

    for copy in firsts_a[2] + firsts_b[2] + firsts_e:
        copy.wait_recv()
    seconds += fold_first(4, 2, 4, 3)
    for copy in seconds:
        copy.wait_recv()
    rows_a, rows_b = (pl.ds(low, high - low) for low, high in SPLITS)
    part[rows_a] = work[rows_a, x, y] + second_a[0] + second_a[1] + second_a[2]
    part[rows_b] = work[rows_b, x, y] + second_b[0] + second_b[1] + second_b[2]
    part[pl.ds(13, 3)] = jnp.zeros((3, 8, DET), jnp.float32)

    thirds = [
        send(part.at[pl.ds(2 * p["z"], 2)], third.at[i - 1], p) for i, p in around("z")
    ]
    for copy in lights + rows_out:
        copy.wait_recv()
    last_row = lax.axis_size("scan") - 1
    for c in range(3):
        added = jnp.where(scan == last_row, 0.0, rows_in[0, c])
        added = added + jnp.where(scan == 0, 0.0, rows_in[1, c])
        own = canvas[c, pl.ds(DET, DET), span] if c < 2 else light_ref[pl.ds(DET, DET), span]
        frame[c] = own + added
    beyond = pl.ds(pl.multiple_of((1 - tile) * 2 * DET, DET), DET)
    sides = copies.send(frame.at[:, :, beyond], cols_in, across_tile)
    mine = part[pl.ds(2 * z, 2)]
    for i, copy in enumerate(thirds):
        copy.wait_recv()
        mine = mine + third[i]
    pair = pl.ds(2 * z, 2)
    both[core, pair] = mine
    backs = [send(both.at[core, pair], both.at[core, pair], p) for i, p in around("z")]
    for copy in backs:
        copy.wait_recv()
    across = send(both.at[core], both.at[core], partner)
    across.wait_recv()

    light = both[0, 12]
    power = jnp.zeros((8, DET), jnp.float32)
    for c in range(2):
        for slot in range(12):
            old = probe_ref[12 * c + slot_channel(slot), x, y]
            power = power + old * old
            block[c, pl.ds(8 * slot, 8)] = old + both[c, slot] / (light + PROBE_REG)
    for i in range(12):
        upd_ref[core, i, x, y] = block[core, pl.ds(8 * i, 8)]
    rows = jnp.concatenate(
        [
            jnp.concatenate([block[c, pl.ds(s, 12, stride=8)] for s in range(8)], axis=1)
            for c in range(2)
        ],
        axis=0,
    )
    padded = jnp.concatenate([rows, jnp.zeros((DET - 24, 8 * DET), jnp.float32)], axis=0)
    line = lax.broadcasted_iota(jnp.int32, (8, DET), 0)
    total = jnp.sum(both[1, 12], axis=0, keepdims=True)
    model = jnp.sum(power * light, axis=0, keepdims=True)
    extra = jnp.where(line == 0, total, jnp.where(line == 1, model, 0.0))
    grams[0, y] = jnp.concatenate([dot32(rows, padded, (1, 1)), extra], axis=0)

    one_a, one_b = pl.ds(0, 6), pl.ds(6, 6)
    gram_y = [send(grams.at[0, y], grams.at[0, y], p) for i, p in around("y")]
    spot_a, spot_b = upd_ref.at[core, one_a, x, y], upd_ref.at[core, one_b, x, y]
    near_a = [send(spot_a, spot_a, p) for i, p in around("y")]
    near_b = [send(spot_b, spot_b, p) for i, p in around("x")]
    for copy in gram_y:
        copy.wait_recv()
    grams[1, x] = (grams[0, 0] + grams[0, 1]) + (grams[0, 2] + grams[0, 3])
    gram_x = [send(grams.at[1, x], grams.at[1, x], p) for i, p in around("x")]
    for copy in near_a:
        copy.wait_recv()
    line_a = upd_ref.at[core, one_a, x]
    far_a = [send(line_a, line_a, p) for i, p in around("x")]
    for copy in near_b:
        copy.wait_recv()
    line_b = upd_ref.at[core, one_b, :, y]
    far_b = [send(line_b, line_b, p) for i, p in around("y")]
    last = [send(line_a, line_a, partner), send(line_b, line_b, partner)]
    for copy in gram_x:
        copy.wait_recv()
    mix_ref[...] = expanded(mixing((grams[1, 0] + grams[1, 1]) + (grams[1, 2] + grams[1, 3])))
    sides.wait_recv()
    for c in range(3):
        left = jnp.where(tile == 1, cols_in[c], 0.0)
        right = jnp.where(tile == 0, cols_in[c], 0.0)
        own = frame[c, :, pl.ds(pl.multiple_of(tile * DET, DET), 2 * DET)]
        inside_ref[c] = own + jnp.concatenate([left, right], axis=1)
    for step in range(1, 4):
        far_a[step - 1].wait_recv()
        got = upd_ref.at[core, one_a, lax.rem(x + 4 - step, 4)]
        last.append(send(got, got, partner))
        far_b[step - 1].wait_recv()
        got = upd_ref.at[core, one_b, :, lax.rem(y + 4 - step, 4)]
        last.append(send(got, got, partner))
    for copy in last:
        copy.wait_recv()
    copies.finish()


COPIES = 96


def reduced(local, spectra, tables, probe):
    f32 = jnp.float32
    high, low, patches, extra, light = spectra
    return pl.pallas_call(
        reduce_kernel,
        out_shape=(
            jax.ShapeDtypeStruct((2, 12, 4, 4, 8, DET), f32),
            jax.ShapeDtypeStruct((192, 192), f32),
            jax.ShapeDtypeStruct((3, DET, 2 * DET), f32),
        ),
        in_specs=[SMEM] + [VMEM] * 7,
        cost_estimate=cost(45),
        out_specs=(VMEM,) * 3,
        scratch_shapes=[
            pltpu.VMEM((12, 4, 4, 8, DET), f32),
            pltpu.VMEM((13, 4, 4, 8, DET), f32),
            pltpu.VMEM((13, 4, 4, 8, DET), f32),
            pltpu.VMEM((4, 2, DET, DET), f32),
            pltpu.VMEM((4, 2 * DET, 2 * DET), jnp.bfloat16),
            pltpu.VMEM((4, 2 * DET, 2 * DET), jnp.bfloat16),
            pltpu.VMEM((2, 3 * DET, 4 * DET), f32),
            pltpu.VMEM((3, 6, 4, 8, DET), f32),
            pltpu.VMEM((3, 7, 4, 8, DET), f32),
            pltpu.VMEM((3, 6, 8, DET), f32),
            pltpu.VMEM((3, 7, 8, DET), f32),
            pltpu.VMEM((16, 8, DET), f32),
            pltpu.VMEM((7, 2, 8, DET), f32),
            pltpu.VMEM((2, 16, 8, DET), f32),
            pltpu.VMEM((2, 96, DET), f32),
            pltpu.VMEM((2, 4, 32, DET), f32),
            pltpu.VMEM((2, 3, DET, 3 * DET), f32),
            pltpu.VMEM((3, DET, 3 * DET), f32),
            pltpu.VMEM((3, DET, DET), f32),
            pltpu.SemaphoreType.DMA((COPIES,)),
            pltpu.SemaphoreType.DMA((COPIES,)),
        ],
        compiler_params=pltpu.CompilerParams(
            collective_id=0, has_side_effects=True, vmem_limit_bytes=LIMIT
        ),
        name="reduce_all",
    )(
        local,
        high,
        low,
        patches,
        extra.reshape(2, 4, 4, 8, DET),
        light,
        tables,
        probe.reshape(24, 4, 4, 8, DET),
    )


def mixing(gram):
    size = 24
    row = lax.broadcasted_iota(jnp.int32, (size, size), 0)
    col = lax.broadcasted_iota(jnp.int32, (size, size), 1)
    identity = jnp.where(row == col, 1.0, 0.0)
    even = lax.rem(row, 2) == 0
    turn = jnp.where(even & (col == row + 1), -1.0, jnp.where(~even & (col == row - 1), 1.0, 0.0))
    products = gram[:size, :size]
    embedded = products + dot32(dot32(turn, products), turn, (1, 1))
    frobenius = jnp.sqrt(jnp.sum(embedded * embedded, keepdims=True))
    current = embedded / frobenius
    inverse = identity
    for repeat in range(NS_STEPS):
        factor = 1.5 * identity - 0.5 * dot32(inverse, current)
        current = dot32(current, factor)
        inverse = dot32(factor, inverse)
    total = jnp.sum(gram[size : size + 1], keepdims=True)
    model = jnp.sum(gram[size + 1 : size + 2], keepdims=True)
    ratio = total / (model + TOTAL_EPS)
    diagonal = jnp.sum(embedded * identity, axis=1, keepdims=True)
    return inverse / jnp.sqrt(frobenius) * jnp.sqrt(ratio * diagonal)


def expanded(mix):
    tall = lax.broadcasted_iota(jnp.int32, (192, 24), 0)
    wide = lax.broadcasted_iota(jnp.int32, (192, 24), 1)
    expand = jnp.where(tall // 8 == wide, 1.0, 0.0)
    large = dot32(dot32(expand, mix), expand, (1, 1))
    row = lax.broadcasted_iota(jnp.int32, (192, 192), 0)
    col = lax.broadcasted_iota(jnp.int32, (192, 192), 1)
    return jnp.where(lax.rem(row, 8) == lax.rem(col, 8), large, 0.0)


def finish_kernel(mix_ref, upd_ref, inside_ref, spec_ref, out_ref, new_ref):
    large = mix_ref[...]
    for b in range(0, 16, 2):
        blocks = [upd_ref[:, b + i].reshape(192, DET) for i in range(2)]
        result = dot32(large, jnp.concatenate(blocks, axis=1))
        for i in range(2):
            block = result[:, i * DET : i * DET + DET].reshape(24, 8, DET)
            for c in range(2):
                for slot in range(12):
                    out_ref[12 * c + slot_channel(slot), b + i] = block[12 * c + slot]
    for c in range(2):
        new_ref[c] = spec_ref[c] + inside_ref[c] / (inside_ref[2] + OBJECT_REG)


def finished(mix, updated, inside, specimen):
    return pl.pallas_call(
        finish_kernel,
        out_shape=(
            jax.ShapeDtypeStruct((24, 16, 8, DET), jnp.float32),
            jax.ShapeDtypeStruct(specimen.shape, jnp.float32),
        ),
        in_specs=[VMEM] * 4,
        out_specs=(VMEM, VMEM),
        cost_estimate=cost(3),
        compiler_params=pltpu.CompilerParams(vmem_limit_bytes=LIMIT),
        name="finish",
    )(mix, updated.reshape(24, 16, 8, DET), inside, specimen)


def body(probe_modes, patterns, specimen, offsets):
    local = offsets.T
    extended, tables = extended_of(specimen), split_tables()
    spectra = forward(local, probe_modes, patterns, extended, tables)
    updated, mix, inside = reduced(local, spectra, tables, probe_modes)
    new_probe, new_specimen = finished(mix, updated, inside, specimen)
    return (new_probe.reshape(probe_modes.shape), new_specimen)


def solution(mesh):
    return jax.shard_map(
        body,
        mesh=mesh,
        in_specs=(
            P(),
            P(("scan", "tile"), None, None),
            P(None, "scan", "tile"),
            P(("scan", "tile"), None),
        ),
        out_specs=(P(), P(None, "scan", "tile")),
        check_vma=False,
    )
```
